128 devices in a mesh: dp: 64 (over x, y, z_lo, core), section: 2 (over z_hi).
Axes of the slice: x: 4, y: 4, z: 4 (z_hi: 2, z_lo: 2; z = z_hi * 2 + z_lo), core: 2. Of those that a mesh axis runs over, the one named last changes fastest.
Arguments:
- samples: bfloat16 [512, 512], P('dp'), may hold values from -16 to 16
- targets: bfloat16 [512, 512], P('dp'), may hold values from -16 to 16
- jacobian_targets: bfloat16 [512, 128, 512], P('dp'), may hold values from -0.1796875 to 0.1796875
- directions: int32 [512, 128], P('dp'), may hold values from 0 to 511
- plan: int32 [64, 8], P('dp'), may hold values from 0 to 7, each once within a row
- weights: bfloat16 [2, 512, 8192], P('section'), may hold values from -1 to 1
Outputs:
- gradients: float32 [2, 512, 8192], P('section', 'dp')
The draws below stay inside these ranges and needn't reach their ends.
Inputs may be any that keep to these rules, and one draw needn't show every extreme that they name: `plan`: each row is a permutation of 0 to 7.
All inputs are finite; a program needn't handle non-finite values.
Results may differ from the reference program's by a relative error of at most 0.0034.
Values may be sent and summed in bfloat16 or wider, within the bound.
A program may use at most 128 MiB of HBM per device.

```python
import jax
import jax.numpy as jnp
from jax import lax

REDUCED = 512
WIDTH = 8192
TANGENTS = 128
MICRO = 4
BATCH = 1
POOL = 8
SAMPLES = 512
N_DP = 64


def draw_weights(key, part):
    scales = jnp.array([REDUCED ** (-0.5), WIDTH ** (-0.5)], jnp.float32)[:, None, None]
    base = jnp.clip(jax.random.normal(key, (2, REDUCED, WIDTH), jnp.float32), -4.0, 4.0)
    return (base * scales).astype(jnp.bfloat16)


def place_ends(values, own_key, smallest, largest):
    extent = values.shape
    index_at = [jax.random.randint(jax.random.fold_in(own_key, axis), (), 0, extent[axis]) for axis in range(len(extent))]
    values = values.at[tuple(index_at)].set(smallest)
    longest = extent.index(max(extent))
    index_at[longest] = (index_at[longest] + 1) % extent[longest]
    return values.at[tuple(index_at)].set(largest)


def raised(values, stream_key, source, target, parts, factor):
    owner, partner = [(jnp.arange(values.shape[dim]) // (values.shape[dim] // parts)).reshape([-1 if axis == dim else 1 for axis in range(values.ndim)]) for dim in (source, target)]
    chosen = jax.random.permutation(stream_key, parts)[partner]
    strong = (owner == chosen) | (owner == (partner + parts // 2) % parts)
    return jnp.where(strong, factor * values, values)


def levels(own_key, extent, split, low, largest):
    loudness = 1.0
    for axis_at, parts in split:
        heights = jax.random.uniform(jax.random.fold_in(jax.random.fold_in(own_key, 6), axis_at), (parts,), jnp.float32, low / len(split), largest / len(split))
        loudness = loudness * jnp.repeat(jnp.exp(heights), extent[axis_at] // parts).reshape((-1,) + (1,) * (len(extent) - 1 - axis_at))
    return loudness


def gaussian(stream_key, extent, spread, most, split=(), held_as=jnp.bfloat16):
    loudness = levels(stream_key, extent, split, -0.22, 0.18) if split else 1.0
    result = jax.random.normal(stream_key, extent, jnp.float32) * spread * loudness
    return jnp.minimum(jnp.maximum(result, -most), most).astype(held_as)


def gaussian_with(stream_key, extent, scale, bound, pieces, heavy, kind=jnp.bfloat16):
    entries = scale * jax.random.normal(stream_key, extent, jnp.float32)
    if pieces:
        entries = entries * levels(stream_key, extent, pieces, -0.22, 0.18)
    return jnp.clip(raised(entries, jax.random.fold_in(stream_key, 3), *heavy), -bound, bound).astype(kind)


def setup_inputs(seed: int = 0) -> dict:
    arg_keys = jax.random.split(jax.random.key(seed), 7)
    samples = gaussian_with(arg_keys[0], (SAMPLES, REDUCED), 1.0, 16.0, ((0, 64),), (0, 1, 64, 4.0))
    targets = gaussian_with(arg_keys[1], (SAMPLES, REDUCED), 1.0, 16.0, ((0, 64),), (0, 1, 64, 4.0))
    jacobian_targets = gaussian(arg_keys[2], (SAMPLES, TANGENTS, REDUCED), 0.03, 0.1796875, ((0, 64),))
    directions = place_ends(jax.random.randint(arg_keys[3], (SAMPLES, TANGENTS), 0, REDUCED), jax.random.fold_in(arg_keys[3], 1), 0, REDUCED - 1).astype(jnp.int32)
    plan = jax.vmap(lambda own: jax.random.permutation(own, POOL))(jax.random.split(arg_keys[4], N_DP)).reshape((N_DP, POOL)).astype(jnp.int32)
    weights = draw_weights(jax.random.fold_in(arg_keys[6], 71), 0)
    return dict(samples=samples, targets=targets, jacobian_targets=jacobian_targets, directions=directions, plan=plan, weights=weights)


jacobian_weight = 32.0


def contract_rows(left, right):
    return lax.dot_general(left, right, (((0,), (0,)), ((), ())), preferred_element_type=jnp.float32)


def against_rows(left, right):
    return lax.dot_general(left, right, (((1,), (1,)), ((), ())), preferred_element_type=jnp.float32)


def encoder_parts(inputs, chosen_dirs, w_first):
    linear = jnp.dot(inputs, w_first, preferred_element_type=jnp.float32)
    squash = jax.nn.sigmoid(linear)
    first_slope = squash * (1.0 + linear * (1.0 - squash))
    second_slope = squash * (1.0 - squash) * (2.0 + linear * (1.0 - 2.0 * squash))
    picked = jnp.take(w_first, chosen_dirs, axis=0)
    return linear, squash, first_slope, second_slope, picked


def encoder_forward(encoded):
    linear, squash, first_slope, second_slope, picked = encoded
    hidden = (linear * squash).astype(jnp.bfloat16)
    tangent = (first_slope[:, None, :] * picked.astype(jnp.float32)).astype(jnp.bfloat16)
    return hidden, tangent


def decoder(hidden, tangent, w_last, target_rows, jacobian_rows):
    columns = hidden.shape[1]
    flattened = tangent.reshape(-1, columns)
    output = against_rows(hidden, w_last)
    jacobian = against_rows(flattened, w_last)
    misfit = (output - target_rows.astype(jnp.float32)).astype(jnp.bfloat16)
    jac_misfit = (jacobian_weight * (jacobian - jacobian_rows.reshape(jacobian.shape).astype(jnp.float32))).astype(jnp.bfloat16)
    grad_last = contract_rows(misfit, hidden) + contract_rows(jac_misfit, flattened)
    cotangent = jnp.dot(misfit, w_last, preferred_element_type=jnp.float32).astype(jnp.bfloat16)
    cotangent_tangent = jnp.dot(jac_misfit, w_last, preferred_element_type=jnp.float32).astype(jnp.bfloat16)
    return grad_last, cotangent, cotangent_tangent.reshape(tangent.shape)


def encoder_backward(inputs, chosen_dirs, encoded, cotangent, cotangent_tangent, reduced):
    linear, squash, first_slope, second_slope, picked = encoded
    projected = jnp.sum(cotangent_tangent.astype(jnp.float32) * picked.astype(jnp.float32), axis=1)
    grad_pre = (cotangent.astype(jnp.float32) * first_slope + second_slope * projected).astype(jnp.bfloat16)
    grad_picked = (cotangent_tangent.astype(jnp.float32) * first_slope[:, None, :]).astype(jnp.bfloat16)
    columns = grad_pre.shape[1]
    onehot = (chosen_dirs.reshape(-1)[:, None] == jnp.arange(reduced, dtype=jnp.int32)[None, :]).astype(jnp.bfloat16)
    return contract_rows(inputs, grad_pre) + contract_rows(onehot, grad_picked.reshape(-1, columns))


def reference(samples, targets, jacobian_targets, directions, plan, weights):
    w_first = weights[0]
    w_last = weights[1]
    offsets = jnp.arange(N_DP, dtype=jnp.int32) * POOL
    picked_rows = (plan[:, :MICRO * BATCH].astype(jnp.int32) + offsets[:, None]).reshape(-1).astype(jnp.int32)

    def accumulate(carried, position):
        first_total, last_total = carried
        inputs = lax.dynamic_slice_in_dim(samples, position, 1, 0)
        chosen_dirs = lax.dynamic_slice_in_dim(directions, position, 1, 0)
        target_rows = lax.dynamic_slice_in_dim(targets, position, 1, 0)
        jacobian_rows = lax.dynamic_slice_in_dim(jacobian_targets, position, 1, 0)
        encoded = encoder_parts(inputs, chosen_dirs, w_first)
        hidden, tangent = encoder_forward(encoded)
        grad_last, cotangent, cotangent_tangent = decoder(hidden, tangent, w_last, target_rows, jacobian_rows)
        grad_first = encoder_backward(inputs, chosen_dirs, encoded, cotangent, cotangent_tangent, REDUCED)
        return (first_total + grad_first, last_total + grad_last), None

    cleared = jnp.zeros((REDUCED, WIDTH), jnp.float32)
    totals, unused = lax.scan(accumulate, (cleared, cleared), picked_rows)
    return jnp.stack([totals[0], totals[1]])
```

```python
import jax
import jax.numpy as jnp
from jax import lax
from jax.experimental import pallas as pl
from jax.experimental.pallas import tpu as pltpu
from jax.sharding import Mesh
from jax.sharding import PartitionSpec as P

AXES = ("x", "y", "zl", "c", "zh")
DP = ("x", "y", "zl", "c")
F32 = jnp.float32
BF16 = jnp.bfloat16
MESH = pl.DeviceIdType.MESH

RED = 512
WIDTH = 8192
TAN = 128
MICRO = 4
POOL = 8
PART = WIDTH // 4
HALF = PART // 2
ROWS = 8 * TAN
NC = 512
JAC = 32.0


def nn(a, b):
    return lax.dot_general(a, b, (((1,), (0,)), ((), ())), preferred_element_type=F32)


def nt(a, b):
    return lax.dot_general(a, b, (((1,), (1,)), ((), ())), preferred_element_type=F32)


def kernel(
    plan,
    samples,
    dirs,
    targets,
    jt_hbm,
    w_hbm,
    out,
    wb,
    jt,
    s32,
    d32,
    t32,
    xd,
    e_buf,
    et_buf,
    xt_buf,
    p32,
    pk,
    tan,
    s1,
    s2,
    jac,
    ox,
    sa,
    fa,
    fb,
    ca,
    cb,
    r1,
    r2,
    mb,
    mt,
    mxt,
    mx,
    rbuf,
    ds,
    dr,
    g32,
    gst,
    p1r,
    a32,
    hst,
    p2r,
    fs,
    lsem,
    wss,
    wrs,
    xss,
    xrs,
    rss,
    rrs,
    ass_,
    ars,
    dss,
    drs,
    p1s,
    p1q,
    p2s,
    p2q,
    p3s,
    p3q,
):
    x = lax.axis_index("x")
    y = lax.axis_index("y")
    zl = lax.axis_index("zl")
    c = lax.axis_index("c")
    zh = lax.axis_index("zh")
    z = 2 * zh + zl

    def dev(px=x, py=y, pzl=zl, pc=c, pzh=zh):
        return (px, py, pzl, pc, pzh)

    def xpeer(o):
        return lax.rem(x + o, 4)

    def ypeer(o):
        return lax.rem(y + o, 4)

    n1 = dev(pzl=1 - zl)
    n2 = dev(pzl=1 - zl, pzh=1 - zh)
    mate = dev(pc=1 - c)
    here = dev()

    sends = []

    def send(src, dst, ssem, rsem, where):
        copy = pltpu.make_async_remote_copy(
            src_ref=src, dst_ref=dst, send_sem=ssem, recv_sem=rsem, device_id=where, device_id_type=MESH
        )
        copy.start()
        sends.append(copy)

    def arrived(dst, rsem):
        pltpu.make_async_remote_copy(
            src_ref=dst, dst_ref=dst, send_sem=rsem, recv_sem=rsem, device_id=here, device_id_type=MESH
        ).wait_recv()

    barrier = pltpu.get_barrier_semaphore()
    peers = [n1, n2, dev(pzh=1 - zh)]
    peers += [dev(pzl=a, pc=1 - c, pzh=b) for a in range(2) for b in range(2)]
    peers += [dev(px=xpeer(o)) for o in (1, 2, 3)]
    peers += [dev(py=ypeer(o)) for o in (1, 2, 3)]
    for peer in peers:
        pl.semaphore_signal(barrier, inc=1, device_id=peer, device_id_type=MESH)

    own_w = pltpu.make_async_copy(
        w_hbm.at[0, :, pl.ds(pl.multiple_of(PART * z, PART), PART)], wb.at[zh], lsem.at[0]
    )
    own_w.start()
    own_j = pltpu.make_async_copy(jt_hbm, jt, lsem.at[1])
    own_j.start()

    s32[...] = samples[...].astype(F32)
    d32[...] = dirs[...].astype(F32)
    t32[...] = targets[...].astype(F32)
    xd[zl, MICRO:8, :] = jnp.zeros((8 - MICRO, RED + TAN), F32)
    for i in range(MICRO):
        at = plan[0, i]
        xd[zl, i : i + 1, 0:RED] = s32[pl.ds(at, 1), :]
        xd[zl, i : i + 1, RED : RED + TAN] = d32[pl.ds(at, 1), :]

    pl.semaphore_wait(barrier, len(peers))

    def col(core, kind, place):
        return pl.multiple_of(HALF * core + 512 * kind + 128 * place, 128)

    def wslice(core, kind, place, h):
        return wb.at[1 - zh, pl.ds(256 * h, 256), pl.ds(col(core, kind, place), 128)]

    mine = (x, y)
    for h in range(2):
        for kind in range(2):
            at = col(c, kind, mine[kind])
            send(
                w_hbm.at[0, pl.ds(256 * h, 256), pl.ds(pl.multiple_of(PART * (3 - z) + at, 128), 128)],
                wb.at[zh, pl.ds(256 * h, 256), pl.ds(at, 128)],
                wss.at[h, kind, 0],
                wrs.at[h, kind, 0],
                n2,
            )
    send(xd.at[zl], xd.at[zl], xss.at[0], xrs.at[0], n1)

    for h in range(2):
        for kind in range(2):
            piece = wslice(c, kind, mine[kind], h)
            arrived(piece, wrs.at[h, kind, 0])
            for o in (1, 3, 2):
                to = dev(px=xpeer(o)) if kind == 0 else dev(py=ypeer(o))
                send(piece, piece, wss.at[h, kind, o], wrs.at[h, kind, o], to)
            send(piece, piece, wss.at[h, kind, 4], wrs.at[h, kind, 4], mate)

    arrived(xd.at[1 - zl], xrs.at[0])
    for j in range(8):
        row = xd[j // 4, j % 4 : j % 4 + 1, RED : RED + TAN]
        level = lax.broadcasted_iota(jnp.int32, (RED, TAN), 0).astype(F32)
        hot = jnp.where(level == row, 1.0, 0.0)
        et_buf[:, TAN * j : TAN * (j + 1)] = hot.astype(BF16)
        e_buf[TAN * j : TAN * (j + 1), :] = jnp.transpose(hot).astype(BF16)
    x16 = jnp.concatenate([xd[0, 0:4, 0:RED], xd[1, 0:4, 0:RED], jnp.zeros((8, RED), F32)], axis=0)
    e_buf[ROWS : ROWS + 16, :] = x16.astype(BF16)
    xt_buf[...] = jnp.transpose(x16).astype(BF16)

    for h in range(2):
        for o in (1, 3, 2):
            for kind in range(2):
                piece = wslice(c, kind, lax.rem(mine[kind] + 4 - o, 4), h)
                arrived(piece, wrs.at[h, kind, o])
                send(piece, piece, wss.at[h, kind, 4 + o], wrs.at[h, kind, 4 + o], mate)
    for h in range(2):
        for o in (0, 1, 3, 2):
            for kind in range(2):
                arrived(wslice(1 - c, kind, lax.rem(mine[kind] + 4 - o, 4), h), wrs.at[h, kind, 4 + o])
    own_w.wait()

    jac[...] = jnp.zeros_like(jac)

    @pl.loop(0, PART // NC)
    def _(n):
        cols = pl.ds(pl.multiple_of(n * NC, NC), NC)
        p32[...] = nn(e_buf[...], wb[0, :, cols])
        linear = p32[ROWS : ROWS + 8, :]
        squash = 1.0 / (1.0 + jnp.exp(-linear))
        slope = squash * (1.0 + linear * (1.0 - squash))
        s1[:, cols] = slope
        s2[:, cols] = squash * (1.0 - squash) * (2.0 + linear * (1.0 - 2.0 * squash))
        hidden = jnp.concatenate([linear * squash, jnp.zeros((8, NC), F32)], axis=0)
        tan[ROWS : ROWS + 16, cols] = hidden.astype(BF16)
        for j in range(8):
            rows = slice(TAN * j, TAN * (j + 1))
            picked = p32[rows, :]
            pk[rows, cols] = picked.astype(BF16)
            tan[rows, cols] = (slope[j : j + 1, :] * picked).astype(BF16)
        jac[...] += nt(tan[:, cols], wb[1, :, cols])

    own = 2 * zl + zh
    b1 = 2 * (1 - zl) + zh
    b2 = 2 * (1 - zl) + (1 - zh)
    bo = 2 * zl + (1 - zh)
    for b in range(4):
        o8 = jnp.concatenate([jac[ROWS + 2 * b : ROWS + 2 * b + 2, :], jnp.zeros((14, RED), F32)], axis=0)
        ox[b] = o8
        sa[b, 0:256, :] = jac[256 * b : 256 * b + 256, :].astype(BF16)
        sa[b, 256:272, :] = o8.astype(BF16)
    lo, hi = pl.ds(0, 128), pl.ds(128, 144)
    send(sa.at[bo, lo], fa, rss.at[0], rrs.at[0], n1)
    send(sa.at[bo, hi], fb, rss.at[1], rrs.at[1], n2)
    send(sa.at[b1, lo], r1.at[lo], rss.at[2], rrs.at[2], n1)
    send(sa.at[b2, hi], r2.at[hi], rss.at[3], rrs.at[3], n2)
    arrived(fa, rrs.at[0])
    ca[...] = (sa[b2, 0:128, :].astype(F32) + fa[...].astype(F32)).astype(BF16)
    send(ca, r2.at[lo], rss.at[4], rrs.at[4], n2)
    arrived(fb, rrs.at[1])
    cb[...] = (sa[b1, 128:272, :].astype(F32) + fb[...].astype(F32)).astype(BF16)
    send(cb, r1.at[hi], rss.at[5], rrs.at[5], n1)

    own_j.wait()
    arrived(r1.at[lo], rrs.at[2])
    arrived(r2.at[lo], rrs.at[4])
    p0 = plan[0, 2 * zh]
    p1 = plan[0, 2 * zh + 1]
    full = jac[pl.ds(pl.multiple_of(256 * own, 256), 128), :]
    full = full + r1[0:128, :].astype(F32) + r2[0:128, :].astype(F32)
    mb[own, 0:128, :] = (JAC * (full - jt[p0].astype(F32))).astype(BF16)
    send(mb.at[own, lo], mb.at[own, lo], ass_.at[0], ars.at[0], n1)
    send(mb.at[own, lo], mb.at[own, lo], ass_.at[1], ars.at[1], n2)
    arrived(r2.at[hi], rrs.at[3])
    arrived(r1.at[hi], rrs.at[5])
    full = jac[pl.ds(pl.multiple_of(256 * own + 128, 128), 128), :]
    full = full + r1[128:256, :].astype(F32) + r2[128:256, :].astype(F32)
    mb[own, 128:256, :] = (JAC * (full - jt[p1].astype(F32))).astype(BF16)
    full = ox[own] + r1[256:272, :].astype(F32) + r2[256:272, :].astype(F32)
    goal = jnp.concatenate([t32[pl.ds(p0, 1), :], t32[pl.ds(p1, 1), :], jnp.zeros((14, RED), F32)], axis=0)
    mb[own, 256:272, :] = (full - goal).astype(BF16)
    send(mb.at[own, hi], mb.at[own, hi], ass_.at[2], ars.at[2], n1)
    send(mb.at[own, hi], mb.at[own, hi], ass_.at[3], ars.at[3], n2)
    arrived(mb.at[b1, lo], ars.at[0])
    send(mb.at[b1, lo], mb.at[b1, lo], ass_.at[4], ars.at[4], n2)
    arrived(mb.at[b2, hi], ars.at[3])
    send(mb.at[b2, hi], mb.at[b2, hi], ass_.at[5], ars.at[5], n1)
    arrived(mb.at[b2, lo], ars.at[1])
    arrived(mb.at[b1, hi], ars.at[2])
    arrived(mb.at[bo, lo], ars.at[4])
    arrived(mb.at[bo, hi], ars.at[5])

    for b in range(4):
        mt[:, 256 * b : 256 * b + 256] = jnp.transpose(mb[b, 0:256, :])
    heads = [mb[b, 256:272, :].astype(F32)[0:2, :] for b in range(4)]
    m16 = jnp.concatenate(heads + [jnp.zeros((8, RED), F32)], axis=0)
    mx[...] = m16.astype(BF16)
    mxt[...] = jnp.transpose(m16).astype(BF16)

    def grads(start):
        cols = pl.ds(pl.multiple_of(start, NC), NC)
        last = nn(mt[...], tan[0:ROWS, cols]) + nn(mxt[...], tan[ROWS : ROWS + 16, cols])
        g32[1] = last
        w1 = wb[1, :, cols]
        for b in range(4):
            p32[256 * b : 256 * b + 256, :] = nn(mb[b, 0:256, :], w1)
        cx = nn(mx[...], w1).astype(BF16).astype(F32)
        pre = []
        for j in range(8):
            rows = slice(TAN * j, TAN * (j + 1))
            ct = p32[rows, :].astype(BF16).astype(F32)
            slope = s1[j : j + 1, cols]
            projected = jnp.sum(ct * pk[rows, cols].astype(F32), axis=0, keepdims=True)
            pre.append(cx[j : j + 1, :] * slope + s2[j : j + 1, cols] * projected)
            rbuf[rows, :] = (ct * slope).astype(BF16)
        pre16 = jnp.concatenate(pre + [jnp.zeros((8, NC), F32)], axis=0).astype(BF16)
        g32[0] = nn(et_buf[...], rbuf[...]) + nn(xt_buf[...], pre16)

    lr = 32
    for q in range(4):
        if q < 2:
            grads(HALF * (1 - c) + NC * q)
            ds[q] = g32[...].astype(BF16)
            send(ds.at[q], dr.at[q], dss.at[q], drs.at[q], mate)
            continue
        q = q - 2
        grads(HALF * c + NC * q)
        arrived(dr.at[q], drs.at[q])
        total = g32[...] + dr[q].astype(F32)
        a32[q] = total.reshape(2, 4, 4, lr, NC)
        gst[q] = total.astype(BF16).reshape(2, 4, 4, lr, NC)
        for o in (2, 1, 3):
            if q == 0:
                src, to = gst.at[q, :, xpeer(o)], dev(px=xpeer(o))
            else:
                src, to = gst.at[q, :, :, ypeer(o)], dev(py=ypeer(o))
            send(src, p1r.at[q, o - 1], p1s.at[q, o - 1], p1q.at[q, o - 1], to)

    for q in range(2):
        for o in (1, 3, 2):
            arrived(p1r.at[q, o - 1], p1q.at[q, o - 1])
        total = a32[q, :, x] if q == 0 else a32[q, :, :, y]
        for o in (1, 3, 2):
            total = total + p1r[q, o - 1].astype(F32)
        hst[q] = total.astype(BF16)
        g32[0, 256 * q : 256 * q + 256, :] = total.reshape(256, NC)
        for o in (2, 1, 3):
            if q == 0:
                src, to = hst.at[q, :, ypeer(o)], dev(py=ypeer(o))
            else:
                src, to = hst.at[q, :, xpeer(o)], dev(px=xpeer(o))
            send(src, p2r.at[q, o - 1], p2s.at[q, o - 1], p2q.at[q, o - 1], to)
    for q in range(2):
        for o in (1, 3, 2):
            arrived(p2r.at[q, o - 1], p2q.at[q, o - 1])
        keep = y if q == 0 else x
        for layer in range(2):
            total = g32[0, pl.ds(pl.multiple_of(256 * q + 128 * layer + lr * keep, lr), lr), :]
            for o in (1, 3, 2):
                total = total + p2r[q, o - 1, layer].astype(F32)
            fs[layer, :, NC * q : NC * (q + 1)] = total

    where = pl.ds(pl.multiple_of(PART * z + HALF * c, HALF), HALF)
    me = 2 * z + c
    for dzh in (1, 0):
        for dzl in (1, 0):
            for dc in (1, 0):
                if dzh + dzl + dc == 0:
                    continue
                pzh, pzl, pc = (lax.rem(a + b, 2) for a, b in ((zh, dzh), (zl, dzl), (c, dc)))
                at = pl.multiple_of(16 * pzl + 8 * pc, 8)
                k = 4 * dzh + 2 * dzl + dc - 1
                send(
                    fs.at[pzh, pl.ds(at, 8), :],
                    out.at[:, where],
                    p3s.at[k],
                    p3q.at[k],
                    dev(pzl=pzl, pc=pc, pzh=pzh),
                )
    out[:, where] = fs[zh, pl.ds(pl.multiple_of(16 * zl + 8 * c, 8), 8), :]
    for dzh in (0, 1):
        for dzl in (0, 1):
            for dc in (0, 1):
                if dzh + dzl + dc == 0:
                    continue
                pzh, pzl, pc = (lax.rem(a + b, 2) for a, b in ((zh, dzh), (zl, dzl), (c, dc)))
                k = 4 * dzh + 2 * dzl + dc - 1
                at = pl.multiple_of(PART * (2 * pzh + pzl) + HALF * pc, HALF)
                arrived(out.at[:, pl.ds(at, HALF)], p3q.at[k])
    for copy in sends:
        copy.wait_send()


def shards(samples, targets, jacobian_targets, directions, plan, weights):
    vmem = pl.BlockSpec(memory_space=pltpu.VMEM)
    anywhere = pl.BlockSpec(memory_space=pl.ANY)
    dma = pltpu.SemaphoreType.DMA
    v = pltpu.VMEM
    result = pl.pallas_call(
        kernel,
        out_shape=jax.ShapeDtypeStruct((8, WIDTH), F32),
        in_specs=[pl.BlockSpec(memory_space=pltpu.SMEM), vmem, vmem, vmem, anywhere, anywhere],
        out_specs=vmem,
        scratch_shapes=[
            v((2, RED, PART), BF16),
            v((POOL, TAN, RED), BF16),
            v((POOL, RED), F32),
            v((POOL, TAN), F32),
            v((POOL, RED), F32),
            v((2, 8, RED + TAN), F32),
            v((ROWS + 16, RED), BF16),
            v((RED, ROWS), BF16),
            v((RED, 16), BF16),
            v((ROWS + 16, NC), F32),
            v((ROWS, PART), BF16),
            v((ROWS + 16, PART), BF16),
            v((8, PART), F32),
            v((8, PART), F32),
            v((ROWS + 16, RED), F32),
            v((4, 16, RED), F32),
            v((4, 272, RED), BF16),
            v((128, RED), BF16),
            v((144, RED), BF16),
            v((128, RED), BF16),
            v((144, RED), BF16),
            v((272, RED), BF16),
            v((272, RED), BF16),
            v((4, 272, RED), BF16),
            v((RED, ROWS), BF16),
            v((RED, 16), BF16),
            v((16, RED), BF16),
            v((ROWS, NC), BF16),
            v((2, 2, RED, NC), BF16),
            v((2, 2, RED, NC), BF16),
            v((2, RED, NC), F32),
            v((2, 2, 4, 4, 32, NC), BF16),
            v((2, 3, 2, 4, 32, NC), BF16),
            v((2, 2, 4, 4, 32, NC), F32),
            v((2, 2, 4, 32, NC), BF16),
            v((2, 3, 2, 32, NC), BF16),
            v((2, 32, HALF), F32),
            dma((2,)),
            dma((2, 2, 8)),
            dma((2, 2, 8)),
            dma((1,)),
            dma((1,)),
            dma((6,)),
            dma((6,)),
            dma((6,)),
            dma((6,)),
            dma((2,)),
            dma((2,)),
            dma((2, 3)),
            dma((2, 3)),
            dma((2, 3)),
            dma((2, 3)),
            dma((7,)),
            dma((7,)),
        ],
        compiler_params=pltpu.CompilerParams(
            collective_id=0, has_side_effects=True, vmem_limit_bytes=60 * 1024 * 1024
        ),
        name="step",
    )(plan, samples, directions, targets, jacobian_targets, weights)
    return result[None]


def solution(mesh):
    torus = Mesh(mesh.devices.reshape(4, 4, 2, 2, 2), AXES)
    return jax.shard_map(
        shards,
        mesh=torus,
        in_specs=(
            P(DP, None),
            P(DP, None),
            P(DP, None, None),
            P(DP, None),
            P(DP, None),
            P("zh", None, None),
        ),
        out_specs=P("zh", DP, None),
        check_vma=False,
    )
```

```python
import jax
import jax.numpy as jnp
from jax import lax
from jax.experimental import pallas as pl
from jax.experimental.pallas import tpu as pltpu
from jax.sharding import Mesh
from jax.sharding import PartitionSpec as P

AXES = ("x", "y", "zl", "c", "zh")
DP = ("x", "y", "zl", "c")
F32 = jnp.float32
BF16 = jnp.bfloat16
MESH = pl.DeviceIdType.MESH

RED = 512
WIDTH = 8192
TAN = 128
MICRO = 4
POOL = 8
PART = WIDTH // 4
HALF = PART // 2
ROWS = 8 * TAN
NC = 512
JAC = 32.0


def nn(a, b):
    return lax.dot_general(a, b, (((1,), (0,)), ((), ())), preferred_element_type=F32)


def nt(a, b):
    return lax.dot_general(a, b, (((1,), (1,)), ((), ())), preferred_element_type=F32)


def kernel(
    plan,
    samples_hbm,
    dirs_hbm,
    targets_hbm,
    jt_hbm,
    w_hbm,
    out,
    samples,
    dirs,
    targets,
    wb,
    jt,
    s32,
    d32,
    t32,
    xd,
    e_buf,
    et_buf,
    xt_buf,
    p32,
    pk,
    tan,
    s1,
    s2,
    jac,
    ox,
    sa,
    fa,
    fb,
    ca,
    cb,
    r1,
    r2,
    mb,
    mt,
    mxt,
    lm,
    pr,
    g,
    ds,
    dr,
    gst,
    p1r,
    hst,
    h32,
    p2r,
    fs,
    lsem,
    wss,
    wrs,
    xss,
    xrs,
    rss,
    rrs,
    ass_,
    ars,
    dss,
    drs,
    p1s,
    p1q,
    p2s,
    p2q,
    p3s,
    p3q,
):
    x = lax.axis_index("x")
    y = lax.axis_index("y")
    zl = lax.axis_index("zl")
    c = lax.axis_index("c")
    zh = lax.axis_index("zh")
    z = 2 * zh + zl

    def dev(px=x, py=y, pzl=zl, pc=c, pzh=zh):
        return (px, py, pzl, pc, pzh)

    def xpeer(o):
        return lax.rem(x + o, 4)

    def ypeer(o):
        return lax.rem(y + o, 4)

    n1 = dev(pzl=1 - zl)
    n2 = dev(pzl=1 - zl, pzh=1 - zh)
    mate = dev(pc=1 - c)
    here = dev()

    sends = []

    def send(src, dst, ssem, rsem, where):
        copy = pltpu.make_async_remote_copy(
            src_ref=src, dst_ref=dst, send_sem=ssem, recv_sem=rsem, device_id=where, device_id_type=MESH
        )
        copy.start()
        sends.append(copy)

    def arrived(dst, rsem):
        pltpu.make_async_remote_copy(
            src_ref=dst, dst_ref=dst, send_sem=rsem, recv_sem=rsem, device_id=here, device_id_type=MESH
        ).wait_recv()

    barrier = pltpu.get_barrier_semaphore()
    peers = [n1, n2, dev(pzh=1 - zh)]
    peers += [dev(pzl=a, pc=1 - c, pzh=b) for a in range(2) for b in range(2)]
    peers += [dev(px=xpeer(o)) for o in (1, 2, 3)]
    peers += [dev(py=ypeer(o)) for o in (1, 2, 3)]
    for peer in peers:
        pl.semaphore_signal(barrier, inc=1, device_id=peer, device_id_type=MESH)

    small = []
    for k, (src, dst) in enumerate(((samples_hbm, samples), (dirs_hbm, dirs), (targets_hbm, targets))):
        small.append(pltpu.make_async_copy(src, dst, lsem.at[2 + k]))
        small[-1].start()
    own_w = pltpu.make_async_copy(
        w_hbm.at[0, :, pl.ds(pl.multiple_of(PART * z, PART), PART)], wb.at[zh], lsem.at[0]
    )
    own_w.start()
    own_j = pltpu.make_async_copy(jt_hbm, jt, lsem.at[1])
    own_j.start()

    for copy in small:
        copy.wait()
    s32[...] = samples[...].astype(F32)
    d32[...] = dirs[...].astype(F32)
    t32[...] = targets[...].astype(F32)
    xd[zl, MICRO:8, :] = jnp.zeros((8 - MICRO, RED + TAN), F32)
    for i in range(MICRO):
        at = plan[0, i]
        xd[zl, i : i + 1, 0:RED] = s32[pl.ds(at, 1), :]
        xd[zl, i : i + 1, RED : RED + TAN] = d32[pl.ds(at, 1), :]

    pl.semaphore_wait(barrier, len(peers))

    def col(core, kind, place):
        return pl.multiple_of(HALF * core + 512 * kind + 128 * place, 128)

    def wslice(core, kind, place, h):
        return wb.at[1 - zh, pl.ds(256 * h, 256), pl.ds(col(core, kind, place), 128)]

    mine = (x, y)
    for h in range(2):
        for kind in range(2):
            at = col(c, kind, mine[kind])
            send(
                w_hbm.at[0, pl.ds(256 * h, 256), pl.ds(pl.multiple_of(PART * (3 - z) + at, 128), 128)],
                wb.at[zh, pl.ds(256 * h, 256), pl.ds(at, 128)],
                wss.at[h, kind, 0],
                wrs.at[h, kind, 0],
                n2,
            )
    send(xd.at[zl], xd.at[zl], xss.at[0], xrs.at[0], n1)

    for h in range(2):
        for kind in range(2):
            piece = wslice(c, kind, mine[kind], h)
            arrived(piece, wrs.at[h, kind, 0])
            for o in (1, 3, 2):
                to = dev(px=xpeer(o)) if kind == 0 else dev(py=ypeer(o))
                send(piece, piece, wss.at[h, kind, o], wrs.at[h, kind, o], to)
            send(piece, piece, wss.at[h, kind, 4], wrs.at[h, kind, 4], mate)
        if h == 0:
            arrived(xd.at[1 - zl], xrs.at[0])
            for j in range(8):
                row = xd[j // 4, j % 4 : j % 4 + 1, RED : RED + TAN]
                level = lax.broadcasted_iota(jnp.int32, (RED, TAN), 0).astype(F32)
                hot = jnp.where(level == row, 1.0, 0.0)
                et_buf[:, TAN * j : TAN * (j + 1)] = hot.astype(BF16)
                e_buf[TAN * j : TAN * (j + 1), :] = jnp.transpose(hot).astype(BF16)
            x16 = jnp.concatenate(
                [xd[0, 0:4, 0:RED], xd[1, 0:4, 0:RED], jnp.zeros((8, RED), F32)], axis=0
            )
            e_buf[ROWS : ROWS + 16, :] = x16.astype(BF16)
            xt_buf[...] = jnp.transpose(x16).astype(BF16)
            jac[...] = jnp.zeros_like(jac)
            own_w.wait()

    def relay(h, kind):
        for o in (1, 3, 2):
            piece = wslice(c, kind, lax.rem(mine[kind] + 4 - o, 4), h)
            arrived(piece, wrs.at[h, kind, o])
            send(piece, piece, wss.at[h, kind, 4 + o], wrs.at[h, kind, 4 + o], mate)

    def from_mate(kind):
        for h in range(2):
            for o in (0, 1, 3, 2):
                arrived(wslice(1 - c, kind, lax.rem(mine[kind] + 4 - o, 4), h), wrs.at[h, kind, 4 + o])

    def slopes(linear, cols):
        squash = 1.0 / (1.0 + jnp.exp(-linear))
        slope = squash * (1.0 + linear * (1.0 - squash))
        s1[:, cols] = slope
        s2[:, cols] = squash * (1.0 - squash) * (2.0 + linear * (1.0 - 2.0 * squash))
        hidden = jnp.concatenate([linear * squash, jnp.zeros((8, NC), F32)], axis=0)
        tan[ROWS : ROWS + 16, cols] = hidden.astype(BF16)
        return slope

    def forward(start):
        cols = pl.ds(pl.multiple_of(start, NC), NC)
        p32[...] = nn(e_buf[...], wb[0, :, cols])
        slope = slopes(p32[ROWS : ROWS + 8, :], cols)
        for j in range(8):
            rows = slice(TAN * j, TAN * (j + 1))
            picked = p32[rows, :]
            pk[rows, cols] = picked.astype(BF16)
            tan[rows, cols] = (slope[j : j + 1, :] * picked).astype(BF16)
        jac[...] += nt(tan[:, cols], wb[1, :, cols])

    relay(0, 0)
    relay(0, 1)
    relay(1, 0)
    forward(HALF * c)
    relay(1, 1)
    forward(HALF * c + NC)
    from_mate(0)
    forward(HALF * (1 - c))
    from_mate(1)

    own = 2 * zl + zh
    b1 = 2 * (1 - zl) + zh
    b2 = 2 * (1 - zl) + (1 - zh)
    bo = 2 * zl + (1 - zh)
    lo, hi = pl.ds(0, 128), pl.ds(128, 144)
    cols = pl.ds(pl.multiple_of(HALF * (1 - c) + NC, NC), NC)
    tail16 = slice(ROWS, ROWS + 16)
    slopes(nn(e_buf[tail16, :], wb[0, :, cols])[0:8, :], cols)
    o16 = jac[tail16, :] + nt(tan[tail16, cols], wb[1, :, cols])
    for b in range(4):
        o2 = jnp.concatenate([o16[2 * b : 2 * b + 2, :], jnp.zeros((14, RED), F32)], axis=0)
        ox[b] = o2
        sa[b, 256:272, :] = o2.astype(BF16)
    for b, kind in ((bo, 0), (b1, 1), (b2, 2), (own, 3)):
        rows = pl.ds(pl.multiple_of(256 * b, 256), 256)
        p32[0:256, :] = nn(e_buf[rows, :], wb[0, :, cols])
        for e in range(2):
            half = pl.ds(pl.multiple_of(256 * b + 128 * e, 128), 128)
            picked = p32[128 * e : 128 * e + 128, :]
            pk[half, cols] = picked.astype(BF16)
            tan[half, cols] = (s1[pl.ds(2 * b + e, 1), cols] * picked).astype(BF16)
        done = jac[rows, :] + nt(tan[rows, cols], wb[1, :, cols])
        if kind == 3:
            jac[rows, :] = done
        else:
            sa[b, 0:256, :] = done.astype(BF16)
        if kind == 0:
            send(sa.at[bo, lo], fa, rss.at[0], rrs.at[0], n1)
            send(sa.at[bo, hi], fb, rss.at[1], rrs.at[1], n2)
        elif kind == 1:
            send(sa.at[b1, lo], r1.at[lo], rss.at[2], rrs.at[2], n1)
        elif kind == 2:
            send(sa.at[b2, hi], r2.at[hi], rss.at[3], rrs.at[3], n2)
    arrived(fa, rrs.at[0])
    ca[...] = (sa[b2, 0:128, :].astype(F32) + fa[...].astype(F32)).astype(BF16)
    send(ca, r2.at[lo], rss.at[4], rrs.at[4], n2)
    arrived(fb, rrs.at[1])
    cb[...] = (sa[b1, 128:272, :].astype(F32) + fb[...].astype(F32)).astype(BF16)
    send(cb, r1.at[hi], rss.at[5], rrs.at[5], n1)

    own_j.wait()
    arrived(r1.at[lo], rrs.at[2])
    arrived(r2.at[lo], rrs.at[4])
    p0 = plan[0, 2 * zh]
    p1 = plan[0, 2 * zh + 1]
    full = jac[pl.ds(pl.multiple_of(256 * own, 256), 128), :]
    full = full + r1[0:128, :].astype(F32) + r2[0:128, :].astype(F32)
    mb[own, 0:128, :] = (JAC * (full - jt[p0].astype(F32))).astype(BF16)
    send(mb.at[own, lo], mb.at[own, lo], ass_.at[0], ars.at[0], n1)
    send(mb.at[own, lo], mb.at[own, lo], ass_.at[1], ars.at[1], n2)
    arrived(r2.at[hi], rrs.at[3])
    arrived(r1.at[hi], rrs.at[5])
    full = jac[pl.ds(pl.multiple_of(256 * own + 128, 128), 128), :]
    full = full + r1[128:256, :].astype(F32) + r2[128:256, :].astype(F32)
    mb[own, 128:256, :] = (JAC * (full - jt[p1].astype(F32))).astype(BF16)
    full = ox[own] + r1[256:272, :].astype(F32) + r2[256:272, :].astype(F32)
    goal = jnp.concatenate([t32[pl.ds(p0, 1), :], t32[pl.ds(p1, 1), :], jnp.zeros((14, RED), F32)], axis=0)
    mb[own, 256:272, :] = (full - goal).astype(BF16)
    send(mb.at[own, hi], mb.at[own, hi], ass_.at[2], ars.at[2], n1)
    send(mb.at[own, hi], mb.at[own, hi], ass_.at[3], ars.at[3], n2)

    def ends(pair):
        return [(b, 128 * e, pl.ds(pl.multiple_of(256 * b + 128 * e, 128), 128), 2 * b + e) for b, e in pair]

    def turn(pair):
        for k, (b, at, _, _) in enumerate(ends(pair)):
            mt[:, 128 * k : 128 * k + 128] = jnp.transpose(mb[b, at : at + 128, :])
            lm[128 * k : 128 * k + 128, :] = mb[b, at : at + 128, :]

    def picked_grads(pair, cot, cols):
        parts = []
        for k, (_, _, rows, j) in enumerate(ends(pair)):
            ct = cot[128 * k : 128 * k + 128, :].astype(BF16).astype(F32)
            pr[pl.ds(j, 1), cols] = jnp.sum(ct * pk[rows, cols].astype(F32), axis=0, keepdims=True)
            parts.append((ct * s1[pl.ds(j, 1), cols]).astype(BF16))
        return jnp.concatenate(parts, axis=0)

    def tangents(pair, cols):
        return jnp.concatenate([tan[rows, cols] for _, _, rows, _ in ends(pair)], axis=0)

    def hot_columns(pair):
        return jnp.concatenate([et_buf[:, rows] for _, _, rows, _ in ends(pair)], axis=1)

    def backward(pair, first):
        turn(pair)

        @pl.loop(0, PART // NC)
        def _(n):
            cols = pl.ds(pl.multiple_of(n * NC, NC), NC)
            last = nn(mt[...], tangents(pair, cols))
            g[1, :, cols] = last if first else g[1, :, cols] + last
            p32[0:256, :] = nn(lm[0:256, :], wb[1, :, cols])
            new = nn(hot_columns(pair), picked_grads(pair, p32[0:256, :], cols))
            g[0, :, cols] = new if first else g[0, :, cols] + new

    backward(((own, 0), (own, 1)), True)
    arrived(mb.at[b1, lo], ars.at[0])
    send(mb.at[b1, lo], mb.at[b1, lo], ass_.at[4], ars.at[4], n2)
    arrived(mb.at[b2, lo], ars.at[1])
    backward(((b1, 0), (b2, 0)), False)
    arrived(mb.at[b2, hi], ars.at[3])
    send(mb.at[b2, hi], mb.at[b2, hi], ass_.at[5], ars.at[5], n1)
    arrived(mb.at[b1, hi], ars.at[2])
    backward(((b1, 1), (b2, 1)), False)
    arrived(mb.at[bo, lo], ars.at[4])
    arrived(mb.at[bo, hi], ars.at[5])

    tail = ((bo, 0), (bo, 1))
    turn(tail)
    heads = [mb[b, 256:272, :].astype(F32)[0:2, :] for b in range(4)]
    m16 = jnp.concatenate(heads + [jnp.zeros((8, RED), F32)], axis=0)
    lm[256:272, :] = m16.astype(BF16)
    mxt[...] = jnp.transpose(m16).astype(BF16)
    for half in range(2):
        for q in range(2):
            base = HALF * (1 - c) if half == 0 else HALF * c
            cols = pl.ds(pl.multiple_of(base + NC * q, NC), NC)
            for layer in (1, 0):
                if layer == 1:
                    total = nn(mt[...], tangents(tail, cols)) + nn(mxt[...], tan[tail16, cols])
                else:
                    p32[0:272, :] = nn(lm[...], wb[1, :, cols])
                    r = picked_grads(tail, p32[0:256, :], cols)
                    cx = p32[256:264, :].astype(BF16).astype(F32)
                    pre = cx * s1[:, cols] + s2[:, cols] * pr[:, cols]
                    pre = jnp.concatenate([pre, jnp.zeros((8, NC), F32)], axis=0).astype(BF16)
                    total = nn(hot_columns(tail), r) + nn(xt_buf[...], pre)
                if half == 0:
                    ds[q, layer] = (g[layer, :, cols] + total).astype(BF16)
                    send(ds.at[q, layer], dr.at[q, layer], dss.at[q, layer], drs.at[q, layer], mate)
                    continue
                g[layer, :, cols] += total
                arrived(dr.at[q, layer], drs.at[q, layer])
                total = g[layer, :, cols] + dr[q, layer].astype(F32)
                g[layer, :, cols] = total
                gst[q, layer] = total.astype(BF16).reshape(4, 4, 32, NC)
                for o in (2, 1, 3):
                    if layer == 1:
                        src, to = gst.at[q, layer, xpeer(o)], dev(px=xpeer(o))
                    else:
                        src, to = gst.at[q, layer, :, ypeer(o)], dev(py=ypeer(o))
                    send(
                        src,
                        p1r.at[q, layer, o - 1],
                        p1s.at[q, layer, o - 1],
                        p1q.at[q, layer, o - 1],
                        to,
                    )

    for q in range(2):
        cols = pl.ds(pl.multiple_of(HALF * c + NC * q, NC), NC)
        for layer in (1, 0):
            for o in (1, 3, 2):
                arrived(p1r.at[q, layer, o - 1], p1q.at[q, layer, o - 1])
            for k in range(4):
                rows = 128 * x + 32 * k if layer == 1 else 128 * k + 32 * y
                total = g[layer, pl.ds(pl.multiple_of(rows, 32), 32), cols]
                for o in (1, 3, 2):
                    total = total + p1r[q, layer, o - 1, k].astype(F32)
                hst[q, layer, k] = total.astype(BF16)
                h32[q, layer, k] = total
            for o in (2, 1, 3):
                if layer == 1:
                    src, to = hst.at[q, layer, ypeer(o)], dev(py=ypeer(o))
                else:
                    src, to = hst.at[q, layer, xpeer(o)], dev(px=xpeer(o))
                send(
                    src,
                    p2r.at[q, layer, o - 1],
                    p2s.at[q, layer, o - 1],
                    p2q.at[q, layer, o - 1],
                    to,
                )
    for q in range(2):
        for layer in (1, 0):
            for o in (1, 3, 2):
                arrived(p2r.at[q, layer, o - 1], p2q.at[q, layer, o - 1])
            total = h32[q, layer, y if layer == 1 else x]
            for o in (1, 3, 2):
                total = total + p2r[q, layer, o - 1].astype(F32)
            fs[layer, :, NC * q : NC * (q + 1)] = total

    where = pl.ds(pl.multiple_of(PART * z + HALF * c, HALF), HALF)
    me = 2 * z + c
    for dzh in (1, 0):
        for dzl in (1, 0):
            for dc in (1, 0):
                if dzh + dzl + dc == 0:
                    continue
                pzh, pzl, pc = (lax.rem(a + b, 2) for a, b in ((zh, dzh), (zl, dzl), (c, dc)))
                at = pl.multiple_of(16 * pzl + 8 * pc, 8)
                k = 4 * dzh + 2 * dzl + dc - 1
                send(
                    fs.at[pzh, pl.ds(at, 8), :],
                    out.at[:, where],
                    p3s.at[k],
                    p3q.at[k],
                    dev(pzl=pzl, pc=pc, pzh=pzh),
                )
    out[:, where] = fs[zh, pl.ds(pl.multiple_of(16 * zl + 8 * c, 8), 8), :]
    for dzh in (0, 1):
        for dzl in (0, 1):
            for dc in (0, 1):
                if dzh + dzl + dc == 0:
                    continue
                pzh, pzl, pc = (lax.rem(a + b, 2) for a, b in ((zh, dzh), (zl, dzl), (c, dc)))
                k = 4 * dzh + 2 * dzl + dc - 1
                at = pl.multiple_of(PART * (2 * pzh + pzl) + HALF * pc, HALF)
                arrived(out.at[:, pl.ds(at, HALF)], p3q.at[k])
    for copy in sends:
        copy.wait_send()


def shards(samples, targets, jacobian_targets, directions, plan, weights):
    vmem = pl.BlockSpec(memory_space=pltpu.VMEM)
    anywhere = pl.BlockSpec(memory_space=pl.ANY)
    dma = pltpu.SemaphoreType.DMA
    v = pltpu.VMEM
    result = pl.pallas_call(
        kernel,
        out_shape=jax.ShapeDtypeStruct((8, WIDTH), F32),
        in_specs=[pl.BlockSpec(memory_space=pltpu.SMEM)] + [anywhere] * 5,
        out_specs=vmem,
        scratch_shapes=[
            v((POOL, RED), BF16),
            v((POOL, TAN), jnp.int32),
            v((POOL, RED), BF16),
            v((2, RED, PART), BF16),
            v((POOL, TAN, RED), BF16),
            v((POOL, RED), F32),
            v((POOL, TAN), F32),
            v((POOL, RED), F32),
            v((2, 8, RED + TAN), F32),
            v((ROWS + 16, RED), BF16),
            v((RED, ROWS), BF16),
            v((RED, 16), BF16),
            v((ROWS + 16, NC), F32),
            v((ROWS, PART), BF16),
            v((ROWS + 16, PART), BF16),
            v((8, PART), F32),
            v((8, PART), F32),
            v((ROWS + 16, RED), F32),
            v((4, 16, RED), F32),
            v((4, 272, RED), BF16),
            v((128, RED), BF16),
            v((144, RED), BF16),
            v((128, RED), BF16),
            v((144, RED), BF16),
            v((272, RED), BF16),
            v((272, RED), BF16),
            v((4, 272, RED), BF16),
            v((RED, 256), BF16),
            v((RED, 16), BF16),
            v((272, RED), BF16),
            v((8, PART), F32),
            v((2, RED, PART), F32),
            v((2, 2, RED, NC), BF16),
            v((2, 2, RED, NC), BF16),
            v((2, 2, 4, 4, 32, NC), BF16),
            v((2, 2, 3, 4, 32, NC), BF16),
            v((2, 2, 4, 32, NC), BF16),
            v((2, 2, 4, 32, NC), F32),
            v((2, 2, 3, 32, NC), BF16),
            v((2, 32, HALF), F32),
            dma((5,)),
            dma((2, 2, 8)),
            dma((2, 2, 8)),
            dma((1,)),
            dma((1,)),
            dma((6,)),
            dma((6,)),
            dma((6,)),
            dma((6,)),
            dma((2, 2)),
            dma((2, 2)),
            dma((2, 2, 3)),
            dma((2, 2, 3)),
            dma((2, 2, 3)),
            dma((2, 2, 3)),
            dma((7,)),
            dma((7,)),
        ],
        compiler_params=pltpu.CompilerParams(
            collective_id=0, has_side_effects=True, vmem_limit_bytes=60 * 1024 * 1024
        ),
        name="step",
    )(plan, samples, directions, targets, jacobian_targets, weights)
    return result[None]


def solution(mesh):
    torus = Mesh(mesh.devices.reshape(4, 4, 2, 2, 2), AXES)
    return jax.shard_map(
        shards,
        mesh=torus,
        in_specs=(
            P(DP, None),
            P(DP, None),
            P(DP, None, None),
            P(DP, None),
            P(DP, None),
            P("zh", None, None),
        ),
        out_specs=P("zh", DP, None),
        check_vma=False,
    )
```

```python
import jax
import jax.numpy as jnp
from jax import lax
from jax.experimental import pallas as pl
from jax.experimental.pallas import tpu as pltpu
from jax.sharding import Mesh
from jax.sharding import PartitionSpec as P

AXES = ("x", "y", "zl", "c", "zh")
DP = ("x", "y", "zl", "c")
F32 = jnp.float32
BF16 = jnp.bfloat16
MESH = pl.DeviceIdType.MESH

RED = 512
WIDTH = 8192
TAN = 128
MICRO = 4
POOL = 8
PART = WIDTH // 4
HALF = PART // 2
ROWS = 8 * TAN
NC = 512
JAC = 32.0
LIMIT = 60 * 1024 * 1024


def nn(a, b):
    return lax.dot_general(a, b, (((1,), (0,)), ((), ())), preferred_element_type=F32)


def nt(a, b):
    return lax.dot_general(a, b, (((1,), (1,)), ((), ())), preferred_element_type=F32)


def kernel(
    plan_hbm,
    samples_hbm,
    dirs_hbm,
    targets_hbm,
    jt_hbm,
    w_hbm,
    out,
    plan,
    samples,
    dirs,
    targets,
    wst,
    wb,
    jt,
    s32,
    d32,
    t32,
    xd,
    e_buf,
    et_buf,
    xt_buf,
    p32,
    pk,
    tan,
    s1,
    s2,
    jac,
    ox,
    sa,
    fa,
    fb,
    ca,
    cb,
    r1,
    r2,
    mb,
    mt,
    mxt,
    lm,
    pr,
    g,
    ds,
    dr,
    gst,
    f1,
    cmb,
    p1r,
    hst,
    h32,
    p2r,
    fs,
    like,
    lsem,
    wss,
    wrs,
    xss,
    xrs,
    rss,
    rrs,
    ass_,
    ars,
    dss,
    drs,
    p1s,
    p1q,
    p2s,
    p2q,
    p3s,
    p3q,
):
    x = lax.axis_index("x")
    y = lax.axis_index("y")
    zl = lax.axis_index("zl")
    c = lax.axis_index("c")
    zh = lax.axis_index("zh")
    z = 2 * zh + zl

    def dev(px=x, py=y, pzl=zl, pc=c, pzh=zh):
        return (px, py, pzl, pc, pzh)

    def xpeer(o):
        return lax.rem(x + o, 4)

    def ypeer(o):
        return lax.rem(y + o, 4)

    n1 = dev(pzl=1 - zl)
    n2 = dev(pzl=1 - zl, pzh=1 - zh)
    mate = dev(pc=1 - c)
    here = dev()

    def send(src, dst, ssem, rsem, where):
        copy = pltpu.make_async_remote_copy(
            src_ref=src, dst_ref=dst, send_sem=ssem, recv_sem=rsem, device_id=where, device_id_type=MESH
        )
        copy.start()

    def arrived(dst, rsem):
        pltpu.make_async_remote_copy(
            src_ref=dst, dst_ref=dst, send_sem=rsem, recv_sem=rsem, device_id=here, device_id_type=MESH
        ).wait_recv()

    def sent(like, ssem):
        pltpu.make_async_remote_copy(
            src_ref=like, dst_ref=like, send_sem=ssem, recv_sem=ssem, device_id=here, device_id_type=MESH
        ).wait_send()

    barrier = pltpu.get_barrier_semaphore()
    peers = [n1, n2, dev(pzh=1 - zh)]
    peers += [dev(pzl=a, pc=1 - c, pzh=b) for a in range(2) for b in range(2)]
    peers += [dev(px=xpeer(o)) for o in (1, 2, 3)]
    peers += [dev(py=ypeer(o)) for o in (1, 2, 3)]
    for peer in peers:
        pl.semaphore_signal(barrier, inc=1, device_id=peer, device_id_type=MESH)

    small = []
    pieces = ((plan_hbm, plan), (samples_hbm, samples), (dirs_hbm, dirs), (targets_hbm, targets))
    for k, (src, dst) in enumerate(pieces):
        small.append(pltpu.make_async_copy(src, dst, lsem.at[2 + k]))
        small[-1].start()
    mine = (x, y)
    for k in range(4):
        for kind in range(2):
            first = pl.multiple_of(PART * (3 - z) + 512 * k + 256 * c + 128 * kind, 128)
            src = w_hbm.at[0, pl.ds(pl.multiple_of(128 * mine[kind], 128), 128), pl.ds(first, 128)]
            pltpu.make_async_copy(src, wst.at[k, kind], lsem.at[6]).start()
    own_w = pltpu.make_async_copy(
        w_hbm.at[0, :, pl.ds(pl.multiple_of(PART * z, PART), PART)], wb.at[zh], lsem.at[0]
    )
    own_w.start()
    own_j = pltpu.make_async_copy(jt_hbm, jt, lsem.at[1])
    own_j.start()

    for copy in small:
        copy.wait()
    s32[...] = samples[...].astype(F32)
    d32[...] = dirs[...].astype(F32)
    t32[...] = targets[...].astype(F32)
    xd[zl, MICRO:8, :] = jnp.zeros((8 - MICRO, RED + TAN), F32)
    for i in range(MICRO):
        at = plan[0, i]
        xd[zl, i : i + 1, 0:RED] = s32[pl.ds(at, 1), :]
        xd[zl, i : i + 1, RED : RED + TAN] = d32[pl.ds(at, 1), :]

    pltpu.make_async_copy(wst, wst, lsem.at[6]).wait()
    pl.semaphore_wait(barrier, len(peers))

    def wslice(layer, core, k, kind, place):
        rows = pl.ds(pl.multiple_of(128 * place, 128), 128)
        return wb.at[layer, rows, pl.ds(pl.multiple_of(512 * k + 256 * core + 128 * kind, 128), 128)]

    for k in range(4):
        for kind in range(2):
            send(
                wst.at[k, kind],
                wslice(zh, c, k, kind, mine[kind]),
                wss.at[0],
                wrs.at[2 * k + kind],
                n2,
            )
        if k == 0:
            send(xd.at[zl], xd.at[zl], xss.at[0], xrs.at[0], n1)

    def from_z(k):
        for kind in range(2):
            piece = wslice(1 - zh, c, k, kind, mine[kind])
            arrived(piece, wrs.at[2 * k + kind])
            for o in (1, 3, 2):
                to = dev(px=xpeer(o)) if kind == 0 else dev(py=ypeer(o))
                send(piece, piece, wss.at[0], wrs.at[8 + 2 * k + (o == 2)], to)
            send(piece, piece, wss.at[0], wrs.at[16 + k], mate)

    def relay(k):
        for group in ((1, 3), (2,)):
            arrived(wb.at[1 - zh, pl.ds(0, 128), pl.ds(0, 256 * len(group))], wrs.at[8 + 2 * k + len(group) % 2])
            for o in group:
                for kind in range(2):
                    piece = wslice(1 - zh, c, k, kind, lax.rem(mine[kind] + 4 - o, 4))
                    send(piece, piece, wss.at[0], wrs.at[16 + k], mate)

    def from_mate(k):
        arrived(wb.at[1 - zh, :, pl.ds(pl.multiple_of(512 * k + 256 * (1 - c), 256), 256)], wrs.at[16 + k])

    from_z(0)
    from_z(1)
    arrived(xd.at[1 - zl], xrs.at[0])
    for j in range(8):
        row = xd[j // 4, j % 4 : j % 4 + 1, RED : RED + TAN]
        level = lax.broadcasted_iota(jnp.int32, (RED, TAN), 0).astype(F32)
        hot = jnp.where(level == row, 1.0, 0.0)
        et_buf[:, TAN * j : TAN * (j + 1)] = hot.astype(BF16)
        e_buf[TAN * j : TAN * (j + 1), :] = jnp.transpose(hot).astype(BF16)
    x16 = jnp.concatenate([xd[0, 0:4, 0:RED], xd[1, 0:4, 0:RED], jnp.zeros((8, RED), F32)], axis=0)
    e_buf[ROWS : ROWS + 16, :] = x16.astype(BF16)
    xt_buf[...] = jnp.transpose(x16).astype(BF16)
    jac[...] = jnp.zeros_like(jac)
    own_w.wait()

    def slopes(linear, cols):
        squash = 1.0 / (1.0 + jnp.exp(-linear))
        slope = squash * (1.0 + linear * (1.0 - squash))
        s1[:, cols] = slope
        s2[:, cols] = squash * (1.0 - squash) * (2.0 + linear * (1.0 - 2.0 * squash))
        hidden = jnp.concatenate([linear * squash, jnp.zeros((8, NC), F32)], axis=0)
        tan[ROWS : ROWS + 16, cols] = hidden.astype(BF16)
        return slope

    def forward(start):
        cols = pl.ds(pl.multiple_of(start, NC), NC)
        p32[...] = nn(e_buf[...], wb[0, :, cols])
        slope = slopes(p32[ROWS : ROWS + 8, :], cols)
        for j in range(8):
            rows = slice(TAN * j, TAN * (j + 1))
            picked = p32[rows, :]
            pk[rows, cols] = picked.astype(BF16)
            tan[rows, cols] = (slope[j : j + 1, :] * picked).astype(BF16)
        jac[...] += nt(tan[:, cols], wb[1, :, cols])

    from_z(2)
    relay(0)
    from_z(3)
    relay(1)
    from_mate(0)
    forward(0)
    relay(2)
    from_mate(1)
    forward(NC)
    relay(3)
    from_mate(2)
    forward(2 * NC)
    from_mate(3)

    own = 2 * zl + zh
    b1 = 2 * (1 - zl) + zh
    b2 = 2 * (1 - zl) + (1 - zh)
    bo = 2 * zl + (1 - zh)
    lo, hi = pl.ds(0, 128), pl.ds(128, 144)
    cols = pl.ds(3 * NC, NC)
    tail16 = slice(ROWS, ROWS + 16)
    slopes(nn(e_buf[tail16, :], wb[0, :, cols])[0:8, :], cols)
    o16 = jac[tail16, :] + nt(tan[tail16, cols], wb[1, :, cols])
    for b in range(4):
        o2 = jnp.concatenate([o16[2 * b : 2 * b + 2, :], jnp.zeros((14, RED), F32)], axis=0)
        ox[b] = o2
        sa[b, 256:272, :] = o2.astype(BF16)
    for b, kind in ((bo, 0), (b1, 1), (b2, 2), (own, 3)):
        rows = pl.ds(pl.multiple_of(256 * b, 256), 256)
        p32[0:256, :] = nn(e_buf[rows, :], wb[0, :, cols])
        for e in range(2):
            half = pl.ds(pl.multiple_of(256 * b + 128 * e, 128), 128)
            picked = p32[128 * e : 128 * e + 128, :]
            pk[half, cols] = picked.astype(BF16)
            tan[half, cols] = (s1[pl.ds(2 * b + e, 1), cols] * picked).astype(BF16)
        done = jac[rows, :] + nt(tan[rows, cols], wb[1, :, cols])
        if kind == 3:
            jac[rows, :] = done
        else:
            sa[b, 0:256, :] = done.astype(BF16)
        if kind == 0:
            send(sa.at[bo, lo], fa, rss.at[0], rrs.at[0], n1)
            send(sa.at[bo, hi], fb, rss.at[0], rrs.at[1], n2)
        elif kind == 1:
            send(sa.at[b1, lo], r1.at[lo], rss.at[0], rrs.at[2], n1)
        elif kind == 2:
            send(sa.at[b2, hi], r2.at[hi], rss.at[0], rrs.at[3], n2)
    arrived(fa, rrs.at[0])
    ca[...] = (sa[b2, 0:128, :].astype(F32) + fa[...].astype(F32)).astype(BF16)
    send(ca, r2.at[lo], rss.at[0], rrs.at[4], n2)
    arrived(fb, rrs.at[1])
    cb[...] = (sa[b1, 128:272, :].astype(F32) + fb[...].astype(F32)).astype(BF16)
    send(cb, r1.at[hi], rss.at[0], rrs.at[5], n1)

    own_j.wait()
    arrived(r1.at[lo], rrs.at[2])
    arrived(r2.at[lo], rrs.at[4])
    p0 = plan[0, 2 * zh]
    p1 = plan[0, 2 * zh + 1]
    full = jac[pl.ds(pl.multiple_of(256 * own, 256), 128), :]
    full = full + r1[0:128, :].astype(F32) + r2[0:128, :].astype(F32)
    mb[own, 0:128, :] = (JAC * (full - jt[p0].astype(F32))).astype(BF16)
    send(mb.at[own, lo], mb.at[own, lo], ass_.at[0], ars.at[0], n1)
    arrived(r2.at[hi], rrs.at[3])
    arrived(r1.at[hi], rrs.at[5])
    full = jac[pl.ds(pl.multiple_of(256 * own + 128, 128), 128), :]
    full = full + r1[128:256, :].astype(F32) + r2[128:256, :].astype(F32)
    mb[own, 128:256, :] = (JAC * (full - jt[p1].astype(F32))).astype(BF16)
    full = ox[own] + r1[256:272, :].astype(F32) + r2[256:272, :].astype(F32)
    goal = jnp.concatenate([t32[pl.ds(p0, 1), :], t32[pl.ds(p1, 1), :], jnp.zeros((14, RED), F32)], axis=0)
    mb[own, 256:272, :] = (full - goal).astype(BF16)
    send(mb.at[own, hi], mb.at[own, hi], ass_.at[0], ars.at[3], n2)
    send(mb.at[own, lo], mb.at[own, lo], ass_.at[0], ars.at[1], n2)
    send(mb.at[own, hi], mb.at[own, hi], ass_.at[0], ars.at[2], n1)

    def ends(pair):
        return [(b, 128 * e, pl.ds(pl.multiple_of(256 * b + 128 * e, 128), 128), 2 * b + e) for b, e in pair]

    def turn(pair):
        for k, (b, at, _, _) in enumerate(ends(pair)):
            mt[:, 128 * k : 128 * k + 128] = jnp.transpose(mb[b, at : at + 128, :])
            lm[128 * k : 128 * k + 128, :] = mb[b, at : at + 128, :]

    def picked_grads(pair, cot, cols):
        parts = []
        for k, (_, _, rows, j) in enumerate(ends(pair)):
            ct = cot[128 * k : 128 * k + 128, :].astype(BF16).astype(F32)
            pr[pl.ds(j, 1), cols] = jnp.sum(ct * pk[rows, cols].astype(F32), axis=0, keepdims=True)
            parts.append((ct * s1[pl.ds(j, 1), cols]).astype(BF16))
        return jnp.concatenate(parts, axis=0)

    def tangents(pair, cols):
        return jnp.concatenate([tan[rows, cols] for _, _, rows, _ in ends(pair)], axis=0)

    def hot_columns(pair):
        return jnp.concatenate([et_buf[:, rows] for _, _, rows, _ in ends(pair)], axis=1)

    def add_to(layer, cols, new, first=False):
        g[layer, :, cols] = new if first else g[layer, :, cols] + new

    def backward(pair, first):
        turn(pair)
        chunks = [pl.ds(NC * n, NC) for n in range(PART // NC)]

        def cotangents(n):
            p32[512 * (n % 2) : 512 * (n % 2) + 256, :] = nn(lm[0:256, :], wb[1, :, chunks[n]])

        cotangents(0)
        for n, cols in enumerate(chunks):
            if n + 1 < len(chunks):
                cotangents(n + 1)
            add_to(1, cols, nn(mt[...], tangents(pair, cols)), first)
            r = picked_grads(pair, p32[512 * (n % 2) : 512 * (n % 2) + 256, :], cols)
            add_to(0, cols, nn(hot_columns(pair), r), first)

    backward(((own, 0), (own, 1)), True)
    arrived(mb.at[b1, lo], ars.at[0])
    send(mb.at[b1, lo], mb.at[b1, lo], ass_.at[0], ars.at[4], n2)
    arrived(mb.at[b2, hi], ars.at[3])
    send(mb.at[b2, hi], mb.at[b2, hi], ass_.at[0], ars.at[5], n1)
    backward(((b1, 0), (b2, 1)), False)
    arrived(mb.at[b2, lo], ars.at[1])
    arrived(mb.at[b1, hi], ars.at[2])
    backward(((b1, 1), (b2, 0)), False)
    arrived(mb.at[bo, lo], ars.at[4])
    arrived(mb.at[bo, hi], ars.at[5])

    tail = ((bo, 0), (bo, 1))
    turn(tail)
    heads = [mb[b, 256:272, :].astype(F32)[0:2, :] for b in range(4)]
    m16 = jnp.concatenate(heads + [jnp.zeros((8, RED), F32)], axis=0)
    lm[256:272, :] = m16.astype(BF16)
    mxt[...] = jnp.transpose(m16).astype(BF16)

    def ahead(layer):
        return xpeer(1) if layer == 1 else ypeer(1)

    def behind(layer):
        return xpeer(3) if layer == 1 else ypeer(3)

    def at_place(layer, place):
        return dev(px=place) if layer == 1 else dev(py=place)

    def half_for(q, layer, place, part):
        if layer == 1:
            return gst.at[q, layer, place, pl.ds(2 * part, 2)]
        return gst.at[q, layer, pl.ds(2 * part, 2), place]

    def rows_for(layer, place, k):
        at = 128 * place + 32 * k if layer == 1 else 128 * k + 32 * place
        return pl.ds(pl.multiple_of(at, 32), 32)

    def start_unit(q, layer):
        across = xpeer(2) if layer == 1 else ypeer(2)
        up, down = ahead(layer), behind(layer)
        moves = (
            (half_for(q, layer, across, 0), f1.at[q, layer, 0], up),
            (half_for(q, layer, across, 1), f1.at[q, layer, 1], down),
            (half_for(q, layer, up, 1), p1r.at[q, layer, 0, pl.ds(2, 2)], up),
            (half_for(q, layer, down, 0), p1r.at[q, layer, 1, pl.ds(0, 2)], down),
        )
        for k, (src, dst, place) in enumerate(moves):
            send(src, dst, p1s.at[0], p1q.at[q, layer, min(k, 2)], at_place(layer, place))

    def forward_unit(q, layer):
        cols = pl.ds(pl.multiple_of(HALF * c + NC * q, NC), NC)
        for part, place in ((0, ahead(layer)), (1, behind(layer))):
            arrived(f1.at[q, layer, part], p1q.at[q, layer, part])
            for k in range(2):
                total = g[layer, rows_for(layer, place, 2 * part + k), cols]
                cmb[q, layer, part, k] = (total + f1[q, layer, part, k].astype(F32)).astype(BF16)
            send(
                cmb.at[q, layer, part],
                p1r.at[q, layer, part, pl.ds(2 * part, 2)],
                p1s.at[0],
                p1q.at[q, layer, 2],
                at_place(layer, place),
            )

    units = []
    for half in range(2):
        for q in range(2):
            base = HALF * (1 - c) if half == 0 else HALF * c
            units.append((half, q, pl.ds(pl.multiple_of(base + NC * q, NC), NC)))

    def leave(half, q, layer, cols, total):
        if half == 0:
            ds[q, layer] = (g[layer, :, cols] + total).astype(BF16)
            send(ds.at[q, layer], dr.at[q, layer], dss.at[0], drs.at[q, layer], mate)
        else:
            g[layer, :, cols] += total

    def tail_cotangents(n):
        p32[512 * (n % 2) : 512 * (n % 2) + 272, :] = nn(lm[...], wb[1, :, units[n][2]])

    tail_cotangents(0)
    for n, (half, q, cols) in enumerate(units):
        if n + 1 < len(units):
            tail_cotangents(n + 1)
        total = nn(mt[...], tangents(tail, cols)) + nn(mxt[...], tan[tail16, cols])
        leave(half, q, 1, cols, total)
        at = 512 * (n % 2)
        r = picked_grads(tail, p32[at : at + 256, :], cols)
        cx = p32[at + 256 : at + 264, :].astype(BF16).astype(F32)
        pre = cx * s1[:, cols] + s2[:, cols] * pr[:, cols]
        pre = jnp.concatenate([pre, jnp.zeros((8, NC), F32)], axis=0).astype(BF16)
        leave(half, q, 0, cols, nn(hot_columns(tail), r) + nn(xt_buf[...], pre))
        if half == 0:
            continue
        for layer in (1, 0):
            arrived(dr.at[q, layer], drs.at[q, layer])
            total = g[layer, :, cols] + dr[q, layer].astype(F32)
            g[layer, :, cols] = total
            gst[q, layer] = total.astype(BF16).reshape(4, 4, 32, NC)
            start_unit(q, layer)

    for q in range(2):
        for layer in (1, 0):
            forward_unit(q, layer)
    for q in range(2):
        cols = pl.ds(pl.multiple_of(HALF * c + NC * q, NC), NC)
        for layer in (1, 0):
            arrived(p1r.at[q, layer], p1q.at[q, layer, 2])
            for k in range(4):
                total = g[layer, rows_for(layer, x if layer == 1 else y, k), cols]
                for side in range(2):
                    total = total + p1r[q, layer, side, k].astype(F32)
                hst[q, layer, k] = total.astype(BF16)
                h32[q, layer, k] = total
            for o in (2, 1, 3):
                if layer == 1:
                    src, to = hst.at[q, layer, ypeer(o)], dev(py=ypeer(o))
                else:
                    src, to = hst.at[q, layer, xpeer(o)], dev(px=xpeer(o))
                send(
                    src,
                    p2r.at[q, layer, o - 1],
                    p2s.at[0],
                    p2q.at[q, layer],
                    to,
                )

    others = [(a, b, d) for a in (1, 0) for b in (1, 0) for d in (1, 0) if a + b + d]

    def moved(step):
        pzh, pzl, pc = (lax.rem(a + b, 2) for a, b in zip((zh, zl, c), step))
        return pzh, pzl, pc

    def out_at(pzh, pzl, pc, q):
        return pl.ds(pl.multiple_of(PART * (2 * pzh + pzl) + HALF * pc + NC * q, NC), NC)

    for q in range(2):
        for layer in (1, 0):
            arrived(p2r.at[q, layer], p2q.at[q, layer])
            total = h32[q, layer, y if layer == 1 else x]
            for o in (1, 3, 2):
                total = total + p2r[q, layer, o - 1].astype(F32)
            for k in range(4):
                fs[q, layer, k] = total[8 * k : 8 * k + 8, :].astype(BF16)
        for step in others:
            pzh, pzl, pc = moved(step)
            send(
                fs.at[q, pzh, 2 * pzl + pc],
                out.at[:, out_at(zh, zl, c, q)],
                p3s.at[0],
                p3q.at[0],
                dev(pzl=pzl, pc=pc, pzh=pzh),
            )
        pltpu.make_async_copy(fs.at[q, zh, 2 * zl + c], out.at[:, out_at(zh, zl, c, q)], lsem.at[7]).start()
    arrived(like, p3q.at[0])
    pltpu.make_async_copy(fs.at[0, 0, pl.ds(0, 2)], fs.at[0, 0, pl.ds(0, 2)], lsem.at[7]).wait()
    sent(wb.at[0], wss.at[0])
    sent(xd.at[0], xss.at[0])
    sent(sa.at[pl.ds(0, 3)], rss.at[0])
    sent(mb.at[pl.ds(0, 3)], ass_.at[0])
    sent(ds, dss.at[0])
    sent(gst.at[:, :, pl.ds(0, 3)], p1s.at[0])
    sent(p2r, p2s.at[0])
    sent(like, p3s.at[0])


def shards(samples, targets, jacobian_targets, directions, plan, weights):
    anywhere = pl.BlockSpec(memory_space=pl.ANY)
    dma = pltpu.SemaphoreType.DMA
    v = pltpu.VMEM
    result = pl.pallas_call(
        kernel,
        out_shape=jax.ShapeDtypeStruct((8, WIDTH), BF16),
        in_specs=[anywhere] * 6,
        out_specs=anywhere,
        scratch_shapes=[
            pltpu.SMEM((1, POOL), jnp.int32),
            v((POOL, RED), BF16),
            v((POOL, TAN), jnp.int32),
            v((POOL, RED), BF16),
            v((4, 2, 128, 128), BF16),
            v((2, RED, PART), BF16),
            v((POOL, TAN, RED), BF16),
            v((POOL, RED), F32),
            v((POOL, TAN), F32),
            v((POOL, RED), F32),
            v((2, 8, RED + TAN), F32),
            v((ROWS + 16, RED), BF16),
            v((RED, ROWS), BF16),
            v((RED, 16), BF16),
            v((ROWS + 16, NC), F32),
            v((ROWS, PART), BF16),
            v((ROWS + 16, PART), BF16),
            v((8, PART), F32),
            v((8, PART), F32),
            v((ROWS + 16, RED), F32),
            v((4, 16, RED), F32),
            v((4, 272, RED), BF16),
            v((128, RED), BF16),
            v((144, RED), BF16),
            v((128, RED), BF16),
            v((144, RED), BF16),
            v((272, RED), BF16),
            v((272, RED), BF16),
            v((4, 272, RED), BF16),
            v((RED, 256), BF16),
            v((RED, 16), BF16),
            v((272, RED), BF16),
            v((8, PART), F32),
            v((2, RED, PART), F32),
            v((2, 2, RED, NC), BF16),
            v((2, 2, RED, NC), BF16),
            v((2, 2, 4, 4, 32, NC), BF16),
            v((2, 2, 2, 2, 32, NC), BF16),
            v((2, 2, 2, 2, 32, NC), BF16),
            v((2, 2, 2, 4, 32, NC), BF16),
            v((2, 2, 4, 32, NC), BF16),
            v((2, 2, 4, 32, NC), F32),
            v((2, 2, 3, 32, NC), BF16),
            v((2, 2, 4, 8, NC), BF16),
            v((14, 8, NC), BF16),
            dma((8,)),
            dma((1,)),
            dma((20,)),
            dma((1,)),
            dma((1,)),
            dma((1,)),
            dma((6,)),
            dma((1,)),
            dma((6,)),
            dma((1,)),
            dma((2, 2)),
            dma((1,)),
            dma((2, 2, 3)),
            dma((1,)),
            dma((2, 2)),
            dma((1,)),
            dma((1,)),
        ],
        compiler_params=pltpu.CompilerParams(
            collective_id=0, has_side_effects=True, vmem_limit_bytes=LIMIT
        ),
        name="step",
    )(plan, samples, directions, targets, jacobian_targets, weights)
    return result.astype(F32)[None]


def solution(mesh):
    torus = Mesh(mesh.devices.reshape(4, 4, 2, 2, 2), AXES)
    return jax.shard_map(
        shards,
        mesh=torus,
        in_specs=(
            P(DP, None),
            P(DP, None),
            P(DP, None, None),
            P(DP, None),
            P(DP, None),
            P("zh", None, None),
        ),
        out_specs=P("zh", DP, None),
        check_vma=False,
    )
```

```python
import jax
import jax.numpy as jnp
from jax import lax
from jax.experimental import pallas as pl
from jax.experimental.pallas import tpu as pltpu
from jax.sharding import Mesh
from jax.sharding import PartitionSpec as P

AXES = ("x", "y", "zl", "c", "zh")
DP = ("x", "y", "zl", "c")
F32 = jnp.float32
BF16 = jnp.bfloat16
MESH = pl.DeviceIdType.MESH

RED = 512
WIDTH = 8192
TAN = 128
MICRO = 4
POOL = 8
PART = WIDTH // 4
HALF = PART // 2
ROWS = 8 * TAN
NC = 512
JAC = 32.0
LIMIT = 60 * 1024 * 1024


def nn(a, b):
    return lax.dot_general(a, b, (((1,), (0,)), ((), ())), preferred_element_type=F32)


def nt(a, b):
    return lax.dot_general(a, b, (((1,), (1,)), ((), ())), preferred_element_type=F32)


def kernel(
    plan_hbm,
    samples_hbm,
    dirs_hbm,
    targets_hbm,
    jt_hbm,
    w_hbm,
    out,
    plan,
    samples,
    dirs,
    targets,
    wst,
    wb,
    jt,
    s32,
    d32,
    t32,
    xd,
    e_buf,
    et_buf,
    xt_buf,
    p32,
    pk,
    tan,
    s1,
    s2,
    jac,
    ox,
    sa,
    fa,
    fb,
    ca,
    cb,
    r1,
    r2,
    mb,
    mt,
    mxt,
    lm,
    pr,
    g,
    ds,
    dr,
    gst,
    f1,
    cmb,
    p1r,
    hst,
    like,
    lsem,
    wss,
    wrs,
    xss,
    xrs,
    rss,
    rrs,
    ass_,
    ars,
    dss,
    drs,
    p1s,
    p1q,
    p3s,
    p3q,
):
    x = lax.axis_index("x")
    y = lax.axis_index("y")
    zl = lax.axis_index("zl")
    c = lax.axis_index("c")
    zh = lax.axis_index("zh")
    z = 2 * zh + zl

    def dev(px=x, py=y, pzl=zl, pc=c, pzh=zh):
        return (px, py, pzl, pc, pzh)

    def xpeer(o):
        return lax.rem(x + o, 4)

    def ypeer(o):
        return lax.rem(y + o, 4)

    n1 = dev(pzl=1 - zl)
    n2 = dev(pzl=1 - zl, pzh=1 - zh)
    mate = dev(pc=1 - c)
    here = dev()

    def send(src, dst, ssem, rsem, where):
        copy = pltpu.make_async_remote_copy(
            src_ref=src, dst_ref=dst, send_sem=ssem, recv_sem=rsem, device_id=where, device_id_type=MESH
        )
        copy.start()

    def arrived(dst, rsem):
        pltpu.make_async_remote_copy(
            src_ref=dst, dst_ref=dst, send_sem=rsem, recv_sem=rsem, device_id=here, device_id_type=MESH
        ).wait_recv()

    def sent(like, ssem):
        pltpu.make_async_remote_copy(
            src_ref=like, dst_ref=like, send_sem=ssem, recv_sem=ssem, device_id=here, device_id_type=MESH
        ).wait_send()

    barrier = pltpu.get_barrier_semaphore()
    peers = [n1, n2, dev(pzh=1 - zh)]
    peers += [dev(px=xpeer(o)) for o in (1, 2, 3)]
    peers += [dev(py=ypeer(o)) for o in (1, 2, 3)]
    peers += [dev(pzl=a, pc=1 - c, pzh=b) for a in (zl, 1 - zl) for b in (zh, 1 - zh)]
    for peer in peers:
        pl.semaphore_signal(barrier, inc=1, device_id=peer, device_id_type=MESH)

    small = []
    pieces = ((plan_hbm, plan), (samples_hbm, samples), (dirs_hbm, dirs), (targets_hbm, targets))
    for k, (src, dst) in enumerate(pieces):
        small.append(pltpu.make_async_copy(src, dst, lsem.at[2 + k]))
        small[-1].start()
    mine = (x, y)
    for k in range(4):
        for kind in range(2):
            first = pl.multiple_of(PART * (3 - z) + 1024 * (k // 2) + 512 * c + 256 * (k % 2) + 128 * kind, 128)
            src = w_hbm.at[0, pl.ds(pl.multiple_of(128 * mine[kind], 128), 128), pl.ds(first, 128)]
            pltpu.make_async_copy(src, wst.at[k, kind], lsem.at[6]).start()
    own_w = pltpu.make_async_copy(
        w_hbm.at[0, :, pl.ds(pl.multiple_of(PART * z, PART), PART)], wb.at[zh], lsem.at[0]
    )
    own_w.start()
    own_j = pltpu.make_async_copy(jt_hbm, jt, lsem.at[1])
    own_j.start()

    for copy in small:
        copy.wait()
    s32[...] = samples[...].astype(F32)
    d32[...] = dirs[...].astype(F32)
    t32[...] = targets[...].astype(F32)
    xd[zl, MICRO:8, :] = jnp.zeros((8 - MICRO, RED + TAN), F32)
    for i in range(MICRO):
        at = plan[0, i]
        xd[zl, i : i + 1, 0:RED] = s32[pl.ds(at, 1), :]
        xd[zl, i : i + 1, RED : RED + TAN] = d32[pl.ds(at, 1), :]

    pltpu.make_async_copy(wst, wst, lsem.at[6]).wait()
    pl.semaphore_wait(barrier, len(peers))

    def wslice(layer, core, k, kind, place):
        rows = pl.ds(pl.multiple_of(128 * place, 128), 128)
        at = 1024 * (k // 2) + 512 * core + 256 * (k % 2) + 128 * kind
        return wb.at[layer, rows, pl.ds(pl.multiple_of(at, 128), 128)]

    for k in range(4):
        for kind in range(2):
            send(
                wst.at[k, kind],
                wslice(zh, c, k, kind, mine[kind]),
                wss.at[0],
                wrs.at[2 * k + kind],
                n2,
            )
        if k == 0:
            send(xd.at[zl], xd.at[zl], xss.at[0], xrs.at[0], n1)

    def from_z(k):
        for kind in range(2):
            piece = wslice(1 - zh, c, k, kind, mine[kind])
            arrived(piece, wrs.at[2 * k + kind])
            for o in (1, 3, 2):
                to = dev(px=xpeer(o)) if kind == 0 else dev(py=ypeer(o))
                send(piece, piece, wss.at[0], wrs.at[8 + 2 * k + (o == 2)], to)
            send(piece, piece, wss.at[0], wrs.at[16 + k // 2], mate)

    def relay(k):
        for group in ((1, 3), (2,)):
            arrived(wb.at[1 - zh, pl.ds(0, 128), pl.ds(0, 256 * len(group))], wrs.at[8 + 2 * k + len(group) % 2])
            for o in group:
                for kind in range(2):
                    piece = wslice(1 - zh, c, k, kind, lax.rem(mine[kind] + 4 - o, 4))
                    send(piece, piece, wss.at[0], wrs.at[16 + k // 2], mate)

    def chunk_at(n, core):
        return pl.multiple_of(1024 * n + 512 * core, NC)

    def from_mate(n):
        arrived(wb.at[1 - zh, :, pl.ds(chunk_at(n, 1 - c), NC)], wrs.at[16 + n])

    from_z(0)
    from_z(1)
    arrived(xd.at[1 - zl], xrs.at[0])
    for j in range(8):
        row = xd[j // 4, j % 4 : j % 4 + 1, RED : RED + TAN]
        level = lax.broadcasted_iota(jnp.int32, (RED, TAN), 0).astype(F32)
        hot = jnp.where(level == row, 1.0, 0.0)
        et_buf[:, TAN * j : TAN * (j + 1)] = hot.astype(BF16)
        e_buf[TAN * j : TAN * (j + 1), :] = jnp.transpose(hot).astype(BF16)
    x16 = jnp.concatenate([xd[0, 0:4, 0:RED], xd[1, 0:4, 0:RED], jnp.zeros((8, RED), F32)], axis=0)
    e_buf[ROWS : ROWS + 16, :] = x16.astype(BF16)
    xt_buf[...] = jnp.transpose(x16).astype(BF16)
    jac[...] = jnp.zeros_like(jac)
    own_w.wait()

    def slopes(linear, cols):
        squash = 1.0 / (1.0 + jnp.exp(-linear))
        slope = squash * (1.0 + linear * (1.0 - squash))
        s1[:, cols] = slope
        s2[:, cols] = squash * (1.0 - squash) * (2.0 + linear * (1.0 - 2.0 * squash))
        hidden = jnp.concatenate([linear * squash, jnp.zeros((8, NC), F32)], axis=0)
        tan[ROWS : ROWS + 16, cols] = hidden.astype(BF16)
        return slope

    def forward(start):
        cols = pl.ds(pl.multiple_of(start, NC), NC)
        p32[...] = nn(e_buf[...], wb[0, :, cols])
        slope = slopes(p32[ROWS : ROWS + 8, :], cols)
        for j in range(8):
            rows = slice(TAN * j, TAN * (j + 1))
            picked = p32[rows, :]
            pk[rows, cols] = picked.astype(BF16)
            tan[rows, cols] = (slope[j : j + 1, :] * picked).astype(BF16)
        jac[...] += nt(tan[:, cols], wb[1, :, cols])

    from_z(2)
    relay(0)
    from_z(3)
    relay(1)
    forward(chunk_at(0, c))
    relay(2)
    from_mate(0)
    forward(chunk_at(0, 1 - c))
    relay(3)
    forward(chunk_at(1, c))
    from_mate(1)

    own = 2 * zl + zh
    b1 = 2 * (1 - zl) + zh
    b2 = 2 * (1 - zl) + (1 - zh)
    bo = 2 * zl + (1 - zh)
    lo, hi = pl.ds(0, 128), pl.ds(128, 144)
    cols = pl.ds(chunk_at(1, 1 - c), NC)
    tail16 = slice(ROWS, ROWS + 16)
    slopes(nn(e_buf[tail16, :], wb[0, :, cols])[0:8, :], cols)
    o16 = jac[tail16, :] + nt(tan[tail16, cols], wb[1, :, cols])
    for b in range(4):
        o2 = jnp.concatenate([o16[2 * b : 2 * b + 2, :], jnp.zeros((14, RED), F32)], axis=0)
        ox[b] = o2
        sa[b, 256:272, :] = o2.astype(BF16)
    for b, kind in ((bo, 0), (b1, 1), (b2, 2), (own, 3)):
        rows = pl.ds(pl.multiple_of(256 * b, 256), 256)
        p32[0:256, :] = nn(e_buf[rows, :], wb[0, :, cols])
        for e in range(2):
            half = pl.ds(pl.multiple_of(256 * b + 128 * e, 128), 128)
            picked = p32[128 * e : 128 * e + 128, :]
            pk[half, cols] = picked.astype(BF16)
            tan[half, cols] = (s1[pl.ds(2 * b + e, 1), cols] * picked).astype(BF16)
        done = jac[rows, :] + nt(tan[rows, cols], wb[1, :, cols])
        if kind == 3:
            jac[rows, :] = done
        else:
            sa[b, 0:256, :] = done.astype(BF16)
        if kind == 0:
            send(sa.at[bo, lo], fa, rss.at[0], rrs.at[0], n1)
            send(sa.at[bo, hi], fb, rss.at[0], rrs.at[1], n2)
        elif kind == 1:
            send(sa.at[b1, lo], r1.at[lo], rss.at[0], rrs.at[2], n1)
        elif kind == 2:
            send(sa.at[b2, hi], r2.at[hi], rss.at[0], rrs.at[3], n2)
    arrived(fa, rrs.at[0])
    ca[...] = (sa[b2, 0:128, :].astype(F32) + fa[...].astype(F32)).astype(BF16)
    send(ca, r2.at[lo], rss.at[0], rrs.at[4], n2)
    arrived(fb, rrs.at[1])
    cb[...] = (sa[b1, 128:272, :].astype(F32) + fb[...].astype(F32)).astype(BF16)
    send(cb, r1.at[hi], rss.at[0], rrs.at[5], n1)

    own_j.wait()
    arrived(r1.at[lo], rrs.at[2])
    arrived(r2.at[lo], rrs.at[4])
    p0 = plan[0, 2 * zh]
    p1 = plan[0, 2 * zh + 1]
    full = jac[pl.ds(pl.multiple_of(256 * own, 256), 128), :]
    full = full + r1[0:128, :].astype(F32) + r2[0:128, :].astype(F32)
    mb[own, 0:128, :] = (JAC * (full - jt[p0].astype(F32))).astype(BF16)
    send(mb.at[own, lo], mb.at[own, lo], ass_.at[0], ars.at[0], n1)
    arrived(r2.at[hi], rrs.at[3])
    arrived(r1.at[hi], rrs.at[5])
    full = jac[pl.ds(pl.multiple_of(256 * own + 128, 128), 128), :]
    full = full + r1[128:256, :].astype(F32) + r2[128:256, :].astype(F32)
    mb[own, 128:256, :] = (JAC * (full - jt[p1].astype(F32))).astype(BF16)
    full = ox[own] + r1[256:272, :].astype(F32) + r2[256:272, :].astype(F32)
    goal = jnp.concatenate([t32[pl.ds(p0, 1), :], t32[pl.ds(p1, 1), :], jnp.zeros((14, RED), F32)], axis=0)
    mb[own, 256:272, :] = (full - goal).astype(BF16)
    send(mb.at[own, hi], mb.at[own, hi], ass_.at[0], ars.at[3], n2)
    send(mb.at[own, lo], mb.at[own, lo], ass_.at[0], ars.at[1], n2)
    send(mb.at[own, hi], mb.at[own, hi], ass_.at[0], ars.at[2], n1)

    def ends(pair):
        return [(b, 128 * e, pl.ds(pl.multiple_of(256 * b + 128 * e, 128), 128), 2 * b + e) for b, e in pair]

    def turn(pair):
        for k, (b, at, _, _) in enumerate(ends(pair)):
            mt[:, 128 * k : 128 * k + 128] = jnp.transpose(mb[b, at : at + 128, :])
            lm[128 * k : 128 * k + 128, :] = mb[b, at : at + 128, :]

    def picked_grads(pair, cot, cols):
        parts = []
        for k, (_, _, rows, j) in enumerate(ends(pair)):
            ct = cot[128 * k : 128 * k + 128, :].astype(BF16).astype(F32)
            pr[pl.ds(j, 1), cols] = jnp.sum(ct * pk[rows, cols].astype(F32), axis=0, keepdims=True)
            parts.append((ct * s1[pl.ds(j, 1), cols]).astype(BF16))
        return jnp.concatenate(parts, axis=0)

    def tangents(pair, cols):
        return jnp.concatenate([tan[rows, cols] for _, _, rows, _ in ends(pair)], axis=0)

    def hot_columns(pair):
        return jnp.concatenate([et_buf[:, rows] for _, _, rows, _ in ends(pair)], axis=1)

    def add_to(layer, cols, new, first=False):
        g[layer, :, cols] = new if first else g[layer, :, cols] + new

    def backward(pair, first):
        turn(pair)
        chunks = [pl.ds(NC * n, NC) for n in range(PART // NC)]

        def cotangents(n):
            p32[512 * (n % 2) : 512 * (n % 2) + 256, :] = nn(lm[0:256, :], wb[1, :, chunks[n]])

        cotangents(0)
        for n, cols in enumerate(chunks):
            if n + 1 < len(chunks):
                cotangents(n + 1)
            add_to(1, cols, nn(mt[...], tangents(pair, cols)), first)
            r = picked_grads(pair, p32[512 * (n % 2) : 512 * (n % 2) + 256, :], cols)
            add_to(0, cols, nn(hot_columns(pair), r), first)

    backward(((own, 0), (own, 1)), True)
    arrived(mb.at[b1, lo], ars.at[0])
    send(mb.at[b1, lo], mb.at[b1, lo], ass_.at[0], ars.at[4], n2)
    arrived(mb.at[b2, hi], ars.at[3])
    send(mb.at[b2, hi], mb.at[b2, hi], ass_.at[0], ars.at[5], n1)
    backward(((b1, 0), (b2, 1)), False)
    arrived(mb.at[b2, lo], ars.at[1])
    arrived(mb.at[b1, hi], ars.at[2])
    backward(((b1, 1), (b2, 0)), False)
    arrived(mb.at[bo, lo], ars.at[4])
    arrived(mb.at[bo, hi], ars.at[5])

    tail = ((bo, 0), (bo, 1))
    turn(tail)
    heads = [mb[b, 256:272, :].astype(F32)[0:2, :] for b in range(4)]
    m16 = jnp.concatenate(heads + [jnp.zeros((8, RED), F32)], axis=0)
    lm[256:272, :] = m16.astype(BF16)
    mxt[...] = jnp.transpose(m16).astype(BF16)

    def ahead(layer):
        return xpeer(1) if layer == 1 else ypeer(1)

    def behind(layer):
        return xpeer(3) if layer == 1 else ypeer(3)

    def at_place(layer, place):
        return dev(px=place) if layer == 1 else dev(py=place)

    def half_for(q, layer, place, part):
        if layer == 1:
            return gst.at[q, layer, place, pl.ds(2 * part, 2)]
        return gst.at[q, layer, pl.ds(2 * part, 2), place]

    def rows_for(layer, place, k):
        at = 128 * place + 32 * k if layer == 1 else 128 * k + 32 * place
        return pl.ds(pl.multiple_of(at, 32), 32)

    def start_unit(q, layer):
        across = xpeer(2) if layer == 1 else ypeer(2)
        up, down = ahead(layer), behind(layer)
        moves = (
            (half_for(q, layer, across, 0), f1.at[q, layer, 0], up),
            (half_for(q, layer, across, 1), f1.at[q, layer, 1], down),
            (half_for(q, layer, up, 1), p1r.at[q, layer, 0, pl.ds(2, 2)], up),
            (half_for(q, layer, down, 0), p1r.at[q, layer, 1, pl.ds(0, 2)], down),
        )
        for k, (src, dst, place) in enumerate(moves):
            send(src, dst, p1s.at[0], p1q.at[q, layer, min(k, 2)], at_place(layer, place))

    def forward_unit(q, layer):
        cols = pl.ds(pl.multiple_of(HALF * c + NC * q, NC), NC)
        for part, place in ((0, ahead(layer)), (1, behind(layer))):
            arrived(f1.at[q, layer, part], p1q.at[q, layer, part])
            for k in range(2):
                total = g[layer, rows_for(layer, place, 2 * part + k), cols]
                cmb[q, layer, part, k] = (total + f1[q, layer, part, k].astype(F32)).astype(BF16)
            send(
                cmb.at[q, layer, part],
                p1r.at[q, layer, part, pl.ds(2 * part, 2)],
                p1s.at[0],
                p1q.at[q, layer, 2],
                at_place(layer, place),
            )

    units = []
    for half in range(2):
        for q in range(2):
            base = HALF * (1 - c) if half == 0 else HALF * c
            units.append((half, q, pl.ds(pl.multiple_of(base + NC * q, NC), NC)))

    def leave(half, q, layer, cols, total):
        if half == 0:
            ds[q, layer] = (g[layer, :, cols] + total).astype(BF16)
            send(ds.at[q, layer], dr.at[q, layer], dss.at[0], drs.at[q, layer], mate)
        else:
            g[layer, :, cols] += total

    def tail_cotangents(n):
        p32[512 * (n % 2) : 512 * (n % 2) + 272, :] = nn(lm[...], wb[1, :, units[n][2]])

    tail_cotangents(0)
    for n, (half, q, cols) in enumerate(units):
        if n + 1 < len(units):
            tail_cotangents(n + 1)
        total = nn(mt[...], tangents(tail, cols)) + nn(mxt[...], tan[tail16, cols])
        leave(half, q, 1, cols, total)
        at = 512 * (n % 2)
        r = picked_grads(tail, p32[at : at + 256, :], cols)
        cx = p32[at + 256 : at + 264, :].astype(BF16).astype(F32)
        pre = cx * s1[:, cols] + s2[:, cols] * pr[:, cols]
        pre = jnp.concatenate([pre, jnp.zeros((8, NC), F32)], axis=0).astype(BF16)
        leave(half, q, 0, cols, nn(hot_columns(tail), r) + nn(xt_buf[...], pre))
        if half == 0:
            continue
        for layer in (1, 0):
            arrived(dr.at[q, layer], drs.at[q, layer])
            total = g[layer, :, cols] + dr[q, layer].astype(F32)
            g[layer, :, cols] = total
            gst[q, layer] = total.astype(BF16).reshape(4, 4, 32, NC)
            start_unit(q, layer)

    def cols_at(place, q):
        return pl.ds(pl.multiple_of(HALF * place + NC * q, NC), NC)

    for q in range(2):
        for layer in (1, 0):
            forward_unit(q, layer)
    for q in range(2):
        cols = pl.ds(pl.multiple_of(HALF * c + NC * q, NC), NC)
        for layer in (1, 0):
            arrived(p1r.at[q, layer], p1q.at[q, layer, 2])
            for k in range(4):
                total = g[layer, rows_for(layer, x if layer == 1 else y, k), cols]
                for side in range(2):
                    total = total + p1r[q, layer, side, k].astype(F32)
                for part in range(4):
                    hst[q, layer, k, part] = total[8 * part : 8 * part + 8, :].astype(BF16)
            ring = y if layer == 1 else x
            slot = out.at[ring, :, cols_at(2 * z + c, q)]
            for o in (2, 1, 3, 0):
                place = lax.rem(ring + o, 4)
                for a, b in ((1, 1), (1, 0), (0, 1), (0, 0)):
                    pzl, pc = lax.rem(zl + a, 2), lax.rem(c + b, 2)
                    src = hst.at[q, layer, place, 2 * pzl + pc]
                    to = dev(pzl=pzl, pc=pc, pzh=layer)
                    to = (to[0], place, *to[2:]) if layer == 1 else (place, *to[1:])
                    if o + a + b:
                        send(src, slot, p3s.at[0], p3q.at[0], to)
                        continue

                    @pl.when(zh != layer)
                    def _():
                        send(src, slot, p3s.at[0], p3q.at[0], to)

                    @pl.when(zh == layer)
                    def _():
                        pltpu.make_async_copy(src, slot, lsem.at[7]).start()

    arrived(like, p3q.at[0])
    sent(wb.at[0], wss.at[0])
    sent(xd.at[0], xss.at[0])
    sent(sa.at[pl.ds(0, 3)], rss.at[0])
    sent(mb.at[pl.ds(0, 3)], ass_.at[0])
    sent(ds, dss.at[0])
    sent(gst.at[:, :, pl.ds(0, 3)], p1s.at[0])
    sent(like, p3s.at[0])
    pltpu.make_async_copy(like.at[0:2], like.at[0:2], lsem.at[7]).wait()


def shards(samples, targets, jacobian_targets, directions, plan, weights):
    anywhere = pl.BlockSpec(memory_space=pl.ANY)
    dma = pltpu.SemaphoreType.DMA
    v = pltpu.VMEM
    result = pl.pallas_call(
        kernel,
        out_shape=jax.ShapeDtypeStruct((4, 8, WIDTH), BF16),
        in_specs=[anywhere] * 6,
        out_specs=anywhere,
        scratch_shapes=[
            pltpu.SMEM((1, POOL), jnp.int32),
            v((POOL, RED), BF16),
            v((POOL, TAN), jnp.int32),
            v((POOL, RED), BF16),
            v((4, 2, 128, 128), BF16),
            v((2, RED, PART), BF16),
            v((POOL, TAN, RED), BF16),
            v((POOL, RED), F32),
            v((POOL, TAN), F32),
            v((POOL, RED), F32),
            v((2, 8, RED + TAN), F32),
            v((ROWS + 16, RED), BF16),
            v((RED, ROWS), BF16),
            v((RED, 16), BF16),
            v((ROWS + 16, NC), F32),
            v((ROWS, PART), BF16),
            v((ROWS + 16, PART), BF16),
            v((8, PART), F32),
            v((8, PART), F32),
            v((ROWS + 16, RED), F32),
            v((4, 16, RED), F32),
            v((4, 272, RED), BF16),
            v((128, RED), BF16),
            v((144, RED), BF16),
            v((128, RED), BF16),
            v((144, RED), BF16),
            v((272, RED), BF16),
            v((272, RED), BF16),
            v((4, 272, RED), BF16),
            v((RED, 256), BF16),
            v((RED, 16), BF16),
            v((272, RED), BF16),
            v((8, PART), F32),
            v((2, RED, PART), F32),
            v((2, 2, RED, NC), BF16),
            v((2, 2, RED, NC), BF16),
            v((2, 2, 4, 4, 32, NC), BF16),
            v((2, 2, 2, 2, 32, NC), BF16),
            v((2, 2, 2, 2, 32, NC), BF16),
            v((2, 2, 2, 4, 32, NC), BF16),
            v((2, 2, 4, 4, 8, NC), BF16),
            v((62, 8, NC), BF16),
            dma((8,)),
            dma((1,)),
            dma((18,)),
            dma((1,)),
            dma((1,)),
            dma((1,)),
            dma((6,)),
            dma((1,)),
            dma((6,)),
            dma((1,)),
            dma((2, 2)),
            dma((1,)),
            dma((2, 2, 3)),
            dma((1,)),
            dma((1,)),
        ],
        compiler_params=pltpu.CompilerParams(
            collective_id=0, has_side_effects=True, vmem_limit_bytes=LIMIT
        ),
        name="step",
    )(plan, samples, directions, targets, jacobian_targets, weights)
    return sum(result[k].astype(F32) for k in range(4))[None]


def solution(mesh):
    torus = Mesh(mesh.devices.reshape(4, 4, 2, 2, 2), AXES)
    return jax.shard_map(
        shards,
        mesh=torus,
        in_specs=(
            P(DP, None),
            P(DP, None),
            P(DP, None, None),
            P(DP, None),
            P(DP, None),
            P("zh", None, None),
        ),
        out_specs=P("zh", DP, None),
        check_vma=False,
    )
```

```python
import jax
import jax.numpy as jnp
from jax import lax
from jax.experimental import pallas as pl
from jax.experimental.pallas import tpu as pltpu
from jax.sharding import Mesh
from jax.sharding import PartitionSpec as P

AXES = ("x", "y", "zl", "c", "zh")
DP = ("x", "y", "zl", "c")
F32 = jnp.float32
BF16 = jnp.bfloat16
MESH = pl.DeviceIdType.MESH

RED = 512
WIDTH = 8192
TAN = 128
MICRO = 4
POOL = 8
PART = WIDTH // 4
HALF = PART // 2
ROWS = 8 * TAN
NC = 512
JAC = 32.0
LIMIT = 60 * 1024 * 1024


def nn(a, b):
    return lax.dot_general(a, b, (((1,), (0,)), ((), ())), preferred_element_type=F32)


def nt(a, b):
    return lax.dot_general(a, b, (((1,), (1,)), ((), ())), preferred_element_type=F32)


def kernel(
    plan_hbm,
    samples_hbm,
    dirs_hbm,
    targets_hbm,
    jt_hbm,
    w_hbm,
    out,
    plan,
    samples,
    dirs,
    targets,
    wst,
    wb,
    jt,
    s32,
    d32,
    t32,
    xd,
    e_buf,
    et_buf,
    xt_buf,
    p32,
    pk,
    tan,
    s1,
    s2,
    jac,
    ox,
    sa,
    fa,
    fb,
    ca,
    cb,
    r1,
    r2,
    mb,
    mt,
    mxt,
    lm,
    pr,
    g,
    ds,
    dr,
    gst,
    f1,
    cmb,
    p1r,
    hst,
    like,
    lsem,
    wss,
    wrs,
    xss,
    xrs,
    rss,
    rrs,
    ass_,
    ars,
    dss,
    drs,
    p1s,
    p1q,
    p3s,
    p3q,
):
    x = lax.axis_index("x")
    y = lax.axis_index("y")
    zl = lax.axis_index("zl")
    c = lax.axis_index("c")
    zh = lax.axis_index("zh")
    z = 2 * zh + zl

    def dev(px=x, py=y, pzl=zl, pc=c, pzh=zh):
        return (px, py, pzl, pc, pzh)

    def xpeer(o):
        return lax.rem(x + o, 4)

    def ypeer(o):
        return lax.rem(y + o, 4)

    n1 = dev(pzl=1 - zl)
    n2 = dev(pzl=1 - zl, pzh=1 - zh)
    mate = dev(pc=1 - c)
    here = dev()

    def send(src, dst, ssem, rsem, where):
        copy = pltpu.make_async_remote_copy(
            src_ref=src, dst_ref=dst, send_sem=ssem, recv_sem=rsem, device_id=where, device_id_type=MESH
        )
        copy.start()

    def arrived(dst, rsem):
        pltpu.make_async_remote_copy(
            src_ref=dst, dst_ref=dst, send_sem=rsem, recv_sem=rsem, device_id=here, device_id_type=MESH
        ).wait_recv()

    def sent(like, ssem):
        pltpu.make_async_remote_copy(
            src_ref=like, dst_ref=like, send_sem=ssem, recv_sem=ssem, device_id=here, device_id_type=MESH
        ).wait_send()

    barrier = pltpu.get_barrier_semaphore()
    peers = [n1, n2, dev(pzh=1 - zh)]
    peers += [dev(px=xpeer(o)) for o in (1, 2, 3)]
    peers += [dev(py=ypeer(o)) for o in (1, 2, 3)]
    peers += [dev(pzl=a, pc=1 - c, pzh=b) for a in (zl, 1 - zl) for b in (zh, 1 - zh)]
    for peer in peers:
        pl.semaphore_signal(barrier, inc=1, device_id=peer, device_id_type=MESH)

    small = []
    pieces = ((plan_hbm, plan), (samples_hbm, samples), (dirs_hbm, dirs), (targets_hbm, targets))
    for k, (src, dst) in enumerate(pieces):
        small.append(pltpu.make_async_copy(src, dst, lsem.at[2 + k]))
        small[-1].start()
    mine = (x, y)
    for k in range(4):
        for kind in range(2):
            first = pl.multiple_of(PART * (3 - z) + 1024 * (k // 2) + 512 * c + 256 * (k % 2) + 128 * kind, 128)
            src = w_hbm.at[0, pl.ds(pl.multiple_of(128 * mine[kind], 128), 128), pl.ds(first, 128)]
            pltpu.make_async_copy(src, wst.at[k, kind], lsem.at[6]).start()
    own_w = pltpu.make_async_copy(
        w_hbm.at[0, :, pl.ds(pl.multiple_of(PART * z, PART), PART)], wb.at[zh], lsem.at[0]
    )
    own_w.start()
    own_j = pltpu.make_async_copy(jt_hbm, jt, lsem.at[1])
    own_j.start()

    for copy in small:
        copy.wait()
    s32[...] = samples[...].astype(F32)
    d32[...] = dirs[...].astype(F32)
    t32[...] = targets[...].astype(F32)
    xd[zl, MICRO:8, :] = jnp.zeros((8 - MICRO, RED + TAN), F32)
    for i in range(MICRO):
        at = plan[0, i]
        xd[zl, i : i + 1, 0:RED] = s32[pl.ds(at, 1), :]
        xd[zl, i : i + 1, RED : RED + TAN] = d32[pl.ds(at, 1), :]

    pltpu.make_async_copy(wst, wst, lsem.at[6]).wait()
    pl.semaphore_wait(barrier, len(peers))

    def wslice(layer, core, k, kind, place):
        rows = pl.ds(pl.multiple_of(128 * place, 128), 128)
        at = 1024 * (k // 2) + 512 * core + 256 * (k % 2) + 128 * kind
        return wb.at[layer, rows, pl.ds(pl.multiple_of(at, 128), 128)]

    for k in range(4):
        for kind in range(2):
            send(
                wst.at[k, kind],
                wslice(zh, c, k, kind, mine[kind]),
                wss.at[0],
                wrs.at[2 * k + kind],
                n2,
            )
        if k == 0:
            send(xd.at[zl], xd.at[zl], xss.at[0], xrs.at[0], n1)

    def from_z(k):
        for kind in range(2):
            piece = wslice(1 - zh, c, k, kind, mine[kind])
            arrived(piece, wrs.at[2 * k + kind])
            for o in (1, 3, 2):
                to = dev(px=xpeer(o)) if kind == 0 else dev(py=ypeer(o))
                send(piece, piece, wss.at[0], wrs.at[8 + 2 * k + (o == 2)], to)
            send(piece, piece, wss.at[0], wrs.at[16 + k // 2], mate)

    def relay(k):
        for group in ((1, 3), (2,)):
            arrived(wb.at[1 - zh, pl.ds(0, 128), pl.ds(0, 256 * len(group))], wrs.at[8 + 2 * k + len(group) % 2])
            for o in group:
                for kind in range(2):
                    piece = wslice(1 - zh, c, k, kind, lax.rem(mine[kind] + 4 - o, 4))
                    send(piece, piece, wss.at[0], wrs.at[16 + k // 2], mate)

    def chunk_at(n, core):
        return pl.multiple_of(1024 * n + 512 * core, NC)

    def from_mate(n):
        arrived(wb.at[1 - zh, :, pl.ds(chunk_at(n, 1 - c), NC)], wrs.at[16 + n])

    from_z(0)
    from_z(1)
    arrived(xd.at[1 - zl], xrs.at[0])
    for j in range(8):
        row = xd[j // 4, j % 4 : j % 4 + 1, RED : RED + TAN]
        level = lax.broadcasted_iota(jnp.int32, (RED, TAN), 0).astype(F32)
        hot = jnp.where(level == row, 1.0, 0.0)
        et_buf[:, TAN * j : TAN * (j + 1)] = hot.astype(BF16)
        e_buf[TAN * j : TAN * (j + 1), :] = jnp.transpose(hot).astype(BF16)
    x16 = jnp.concatenate([xd[0, 0:4, 0:RED], xd[1, 0:4, 0:RED], jnp.zeros((8, RED), F32)], axis=0)
    e_buf[ROWS : ROWS + 16, :] = x16.astype(BF16)
    xt_buf[...] = jnp.transpose(x16).astype(BF16)
    jac[...] = jnp.zeros_like(jac)
    own_w.wait()

    def slopes(linear, cols):
        squash = 1.0 / (1.0 + jnp.exp(-linear))
        slope = squash * (1.0 + linear * (1.0 - squash))
        s1[:, cols] = slope
        s2[:, cols] = squash * (1.0 - squash) * (2.0 + linear * (1.0 - 2.0 * squash))
        hidden = jnp.concatenate([linear * squash, jnp.zeros((8, NC), F32)], axis=0)
        tan[ROWS : ROWS + 16, cols] = hidden.astype(BF16)
        return slope

    def forward(start):
        cols = pl.ds(pl.multiple_of(start, NC), NC)
        halves = ((512, ROWS + 16), (0, 512))
        for low, high in halves:
            p32[low:high, :] = nn(e_buf[low:high, :], wb[0, :, cols])
        slope = slopes(p32[ROWS : ROWS + 8, :], cols)
        for low, high in halves:
            for j in range(low // TAN, low // TAN + 4):
                rows = slice(TAN * j, TAN * (j + 1))
                picked = p32[rows, :]
                pk[rows, cols] = picked.astype(BF16)
                tan[rows, cols] = (slope[j : j + 1, :] * picked).astype(BF16)
            jac[low:high, :] += nt(tan[low:high, cols], wb[1, :, cols])

    from_z(2)
    relay(0)
    from_z(3)
    relay(1)
    forward(chunk_at(0, c))
    relay(2)
    from_mate(0)
    forward(chunk_at(0, 1 - c))
    relay(3)
    forward(chunk_at(1, c))
    from_mate(1)

    own = 2 * zl + zh
    b1 = 2 * (1 - zl) + zh
    b2 = 2 * (1 - zl) + (1 - zh)
    bo = 2 * zl + (1 - zh)
    lo, hi = pl.ds(0, 128), pl.ds(128, 144)
    cols = pl.ds(chunk_at(1, 1 - c), NC)
    tail16 = slice(ROWS, ROWS + 16)
    for b, kind in ((bo, 0), (b1, 1), (b2, 2), (own, 3)):
        rows = pl.ds(pl.multiple_of(256 * b, 256), 256)
        if kind == 0:
            p32[0:272, :] = nn(jnp.concatenate([e_buf[rows, :], e_buf[tail16, :]], axis=0), wb[0, :, cols])
            slopes(p32[256:264, :], cols)
        else:
            p32[0:256, :] = nn(e_buf[rows, :], wb[0, :, cols])
        for e in range(2):
            half = pl.ds(pl.multiple_of(256 * b + 128 * e, 128), 128)
            picked = p32[128 * e : 128 * e + 128, :]
            pk[half, cols] = picked.astype(BF16)
            tan[half, cols] = (s1[pl.ds(2 * b + e, 1), cols] * picked).astype(BF16)
        if kind == 0:
            both = nt(jnp.concatenate([tan[rows, cols], tan[tail16, cols]], axis=0), wb[1, :, cols])
            done = jac[rows, :] + both[0:256, :]
            o16 = jac[tail16, :] + both[256:272, :]
            for k in range(4):
                o2 = jnp.concatenate([o16[2 * k : 2 * k + 2, :], jnp.zeros((14, RED), F32)], axis=0)
                ox[k] = o2
                sa[k, 256:272, :] = o2.astype(BF16)
        else:
            done = jac[rows, :] + nt(tan[rows, cols], wb[1, :, cols])
        if kind == 3:
            jac[rows, :] = done
        else:
            sa[b, 0:256, :] = done.astype(BF16)
        if kind == 0:
            send(sa.at[bo, lo], fa, rss.at[0], rrs.at[0], n1)
            send(sa.at[bo, hi], fb, rss.at[0], rrs.at[1], n2)
        elif kind == 1:
            send(sa.at[b1, lo], r1.at[lo], rss.at[0], rrs.at[2], n1)
        elif kind == 2:
            send(sa.at[b2, hi], r2.at[hi], rss.at[0], rrs.at[3], n2)
    arrived(fa, rrs.at[0])
    ca[...] = (sa[b2, 0:128, :].astype(F32) + fa[...].astype(F32)).astype(BF16)
    send(ca, r2.at[lo], rss.at[0], rrs.at[4], n2)
    arrived(fb, rrs.at[1])
    cb[...] = (sa[b1, 128:272, :].astype(F32) + fb[...].astype(F32)).astype(BF16)
    send(cb, r1.at[hi], rss.at[0], rrs.at[5], n1)

    own_j.wait()
    arrived(r1.at[lo], rrs.at[2])
    arrived(r2.at[lo], rrs.at[4])
    p0 = plan[0, 2 * zh]
    p1 = plan[0, 2 * zh + 1]
    full = jac[pl.ds(pl.multiple_of(256 * own, 256), 128), :]
    full = full + r1[0:128, :].astype(F32) + r2[0:128, :].astype(F32)
    mb[own, 0:128, :] = (JAC * (full - jt[p0].astype(F32))).astype(BF16)
    send(mb.at[own, lo], mb.at[own, lo], ass_.at[0], ars.at[0], n1)
    arrived(r2.at[hi], rrs.at[3])
    arrived(r1.at[hi], rrs.at[5])
    full = jac[pl.ds(pl.multiple_of(256 * own + 128, 128), 128), :]
    full = full + r1[128:256, :].astype(F32) + r2[128:256, :].astype(F32)
    mb[own, 128:256, :] = (JAC * (full - jt[p1].astype(F32))).astype(BF16)
    full = ox[own] + r1[256:272, :].astype(F32) + r2[256:272, :].astype(F32)
    goal = jnp.concatenate([t32[pl.ds(p0, 1), :], t32[pl.ds(p1, 1), :], jnp.zeros((14, RED), F32)], axis=0)
    mb[own, 256:272, :] = (full - goal).astype(BF16)
    send(mb.at[own, hi], mb.at[own, hi], ass_.at[0], ars.at[3], n2)
    send(mb.at[own, lo], mb.at[own, lo], ass_.at[0], ars.at[1], n2)
    send(mb.at[own, hi], mb.at[own, hi], ass_.at[0], ars.at[2], n1)

    def ends(pair):
        return [(b, 128 * e, pl.ds(pl.multiple_of(256 * b + 128 * e, 128), 128), 2 * b + e) for b, e in pair]

    def turn(pair):
        for k, (b, at, _, _) in enumerate(ends(pair)):
            mt[:, 128 * k : 128 * k + 128] = jnp.transpose(mb[b, at : at + 128, :])
            lm[128 * k : 128 * k + 128, :] = mb[b, at : at + 128, :]

    def picked_grads(pair, cot, cols):
        parts = []
        for k, (_, _, rows, j) in enumerate(ends(pair)):
            ct = cot[128 * k : 128 * k + 128, :].astype(BF16).astype(F32)
            pr[pl.ds(j, 1), cols] = jnp.sum(ct * pk[rows, cols].astype(F32), axis=0, keepdims=True)
            parts.append((ct * s1[pl.ds(j, 1), cols]).astype(BF16))
        return jnp.concatenate(parts, axis=0)

    def tangents(pair, cols):
        return jnp.concatenate([tan[rows, cols] for _, _, rows, _ in ends(pair)], axis=0)

    def hot_columns(pair):
        return jnp.concatenate([et_buf[:, rows] for _, _, rows, _ in ends(pair)], axis=1)

    def add_to(layer, cols, new, first=False):
        g[layer, :, cols] = new if first else g[layer, :, cols] + new

    def backward(pair, first):
        turn(pair)
        chunks = [pl.ds(NC * n, NC) for n in range(PART // NC)]

        def cotangents(n):
            p32[512 * (n % 2) : 512 * (n % 2) + 256, :] = nn(lm[0:256, :], wb[1, :, chunks[n]])

        cotangents(0)
        for n, cols in enumerate(chunks):
            if n + 1 < len(chunks):
                cotangents(n + 1)
            add_to(1, cols, nn(mt[...], tangents(pair, cols)), first)
            r = picked_grads(pair, p32[512 * (n % 2) : 512 * (n % 2) + 256, :], cols)
            add_to(0, cols, nn(hot_columns(pair), r), first)

    backward(((own, 0), (own, 1)), True)
    arrived(mb.at[b1, lo], ars.at[0])
    send(mb.at[b1, lo], mb.at[b1, lo], ass_.at[0], ars.at[4], n2)
    arrived(mb.at[b2, hi], ars.at[3])
    send(mb.at[b2, hi], mb.at[b2, hi], ass_.at[0], ars.at[5], n1)
    backward(((b1, 0), (b2, 1)), False)
    arrived(mb.at[b2, lo], ars.at[1])
    arrived(mb.at[b1, hi], ars.at[2])
    backward(((b1, 1), (b2, 0)), False)
    arrived(mb.at[bo, lo], ars.at[4])
    arrived(mb.at[bo, hi], ars.at[5])

    tail = ((bo, 0), (bo, 1))
    turn(tail)
    heads = [mb[b, 256:272, :].astype(F32)[0:2, :] for b in range(4)]
    m16 = jnp.concatenate(heads + [jnp.zeros((8, RED), F32)], axis=0)
    lm[256:272, :] = m16.astype(BF16)
    mxt[...] = jnp.transpose(m16).astype(BF16)

    def ahead(layer):
        return xpeer(1) if layer == 1 else ypeer(1)

    def behind(layer):
        return xpeer(3) if layer == 1 else ypeer(3)

    def at_place(layer, place):
        return dev(px=place) if layer == 1 else dev(py=place)

    def half_for(q, layer, place, part):
        if layer == 1:
            return gst.at[q, layer, place, pl.ds(2 * part, 2)]
        return gst.at[q, layer, pl.ds(2 * part, 2), place]

    def rows_for(layer, place, k):
        at = 128 * place + 32 * k if layer == 1 else 128 * k + 32 * place
        return pl.ds(pl.multiple_of(at, 32), 32)

    def start_unit(q, layer, steps):
        across = xpeer(2) if layer == 1 else ypeer(2)
        up, down = ahead(layer), behind(layer)
        moves = (
            (half_for(q, layer, across, 0), f1.at[q, layer, 0], up),
            (half_for(q, layer, across, 1), f1.at[q, layer, 1], down),
            (half_for(q, layer, up, 1), p1r.at[q, layer, 0, pl.ds(2, 2)], up),
            (half_for(q, layer, down, 0), p1r.at[q, layer, 1, pl.ds(0, 2)], down),
        )
        for k in steps:
            src, dst, place = moves[k]
            send(src, dst, p1s.at[0], p1q.at[q, layer, min(k, 2)], at_place(layer, place))

    def forward_unit(q, layer):
        cols = pl.ds(pl.multiple_of(HALF * c + NC * q, NC), NC)
        for part, place in ((0, ahead(layer)), (1, behind(layer))):
            arrived(f1.at[q, layer, part], p1q.at[q, layer, part])
            for k in range(2):
                total = g[layer, rows_for(layer, place, 2 * part + k), cols]
                cmb[q, layer, part, k] = (total + f1[q, layer, part, k].astype(F32)).astype(BF16)
            send(
                cmb.at[q, layer, part],
                p1r.at[q, layer, part, pl.ds(2 * part, 2)],
                p1s.at[0],
                p1q.at[q, layer, 2],
                at_place(layer, place),
            )

    units = []
    for half in range(2):
        for q in range(2):
            base = HALF * (1 - c) if half == 0 else HALF * c
            units.append((half, q, pl.ds(pl.multiple_of(base + NC * q, NC), NC)))

    def leave(half, q, layer, cols, total):
        if half == 0:
            ds[q, layer] = (g[layer, :, cols] + total).astype(BF16)
            send(ds.at[q, layer], dr.at[q, layer], dss.at[0], drs.at[q, layer], mate)
        else:
            g[layer, :, cols] += total

    def tail_cotangents(n):
        p32[512 * (n % 2) : 512 * (n % 2) + 272, :] = nn(lm[...], wb[1, :, units[n][2]])

    tail_cotangents(0)
    for n, (half, q, cols) in enumerate(units):
        if n + 1 < len(units):
            tail_cotangents(n + 1)
        total = nn(mt[...], tangents(tail, cols)) + nn(mxt[...], tan[tail16, cols])
        leave(half, q, 1, cols, total)
        at = 512 * (n % 2)
        r = picked_grads(tail, p32[at : at + 256, :], cols)
        cx = p32[at + 256 : at + 264, :].astype(BF16).astype(F32)
        pre = cx * s1[:, cols] + s2[:, cols] * pr[:, cols]
        pre = jnp.concatenate([pre, jnp.zeros((8, NC), F32)], axis=0).astype(BF16)
        leave(half, q, 0, cols, nn(hot_columns(tail), r) + nn(xt_buf[...], pre))
        if half == 0:
            continue
        for layer in (1, 0):
            arrived(dr.at[q, layer], drs.at[q, layer])
            total = g[layer, :, cols] + dr[q, layer].astype(F32)
            g[layer, :, cols] = total
            gst[q, layer] = total.astype(BF16).reshape(4, 4, 32, NC)
            start_unit(q, layer, range(4) if q == 0 else range(2))

    def cols_at(place, q):
        return pl.ds(pl.multiple_of(HALF * place + NC * q, NC), NC)

    for layer in (1, 0):
        forward_unit(0, layer)
        start_unit(1, layer, range(2, 4))
    for layer in (1, 0):
        forward_unit(1, layer)
    for q in range(2):
        cols = pl.ds(pl.multiple_of(HALF * c + NC * q, NC), NC)
        for layer in (1, 0):
            arrived(p1r.at[q, layer], p1q.at[q, layer, 2])
            for k in range(4):
                total = g[layer, rows_for(layer, x if layer == 1 else y, k), cols]
                for side in range(2):
                    total = total + p1r[q, layer, side, k].astype(F32)
                for part in range(4):
                    hst[q, layer, k, part] = total[8 * part : 8 * part + 8, :].astype(BF16)
            ring = y if layer == 1 else x
            slot = out.at[ring, :, cols_at(2 * z + c, q)]
            for o in (2, 1, 3, 0):
                place = lax.rem(ring + o, 4)
                for a, b in ((1, 1), (1, 0), (0, 1), (0, 0)):
                    pzl, pc = lax.rem(zl + a, 2), lax.rem(c + b, 2)
                    src = hst.at[q, layer, place, 2 * pzl + pc]
                    to = dev(pzl=pzl, pc=pc, pzh=layer)
                    to = (to[0], place, *to[2:]) if layer == 1 else (place, *to[1:])
                    if o + a + b:
                        send(src, slot, p3s.at[0], p3q.at[0], to)
                        continue

                    @pl.when(zh != layer)
                    def _():
                        send(src, slot, p3s.at[0], p3q.at[0], to)

                    @pl.when(zh == layer)
                    def _():
                        pltpu.make_async_copy(src, slot, lsem.at[7]).start()

    arrived(like, p3q.at[0])
    sent(wb.at[0], wss.at[0])
    sent(xd.at[0], xss.at[0])
    sent(sa.at[pl.ds(0, 3)], rss.at[0])
    sent(mb.at[pl.ds(0, 3)], ass_.at[0])
    sent(ds, dss.at[0])
    sent(gst.at[:, :, pl.ds(0, 3)], p1s.at[0])
    sent(like, p3s.at[0])
    pltpu.make_async_copy(like.at[0:2], like.at[0:2], lsem.at[7]).wait()


def shards(samples, targets, jacobian_targets, directions, plan, weights):
    anywhere = pl.BlockSpec(memory_space=pl.ANY)
    dma = pltpu.SemaphoreType.DMA
    v = pltpu.VMEM
    result = pl.pallas_call(
        kernel,
        out_shape=jax.ShapeDtypeStruct((4, 8, WIDTH), BF16),
        in_specs=[anywhere] * 6,
        out_specs=anywhere,
        scratch_shapes=[
            pltpu.SMEM((1, POOL), jnp.int32),
            v((POOL, RED), BF16),
            v((POOL, TAN), jnp.int32),
            v((POOL, RED), BF16),
            v((4, 2, 128, 128), BF16),
            v((2, RED, PART), BF16),
            v((POOL, TAN, RED), BF16),
            v((POOL, RED), F32),
            v((POOL, TAN), F32),
            v((POOL, RED), F32),
            v((2, 8, RED + TAN), F32),
            v((ROWS + 16, RED), BF16),
            v((RED, ROWS), BF16),
            v((RED, 16), BF16),
            v((ROWS + 16, NC), F32),
            v((ROWS, PART), BF16),
            v((ROWS + 16, PART), BF16),
            v((8, PART), F32),
            v((8, PART), F32),
            v((ROWS + 16, RED), F32),
            v((4, 16, RED), F32),
            v((4, 272, RED), BF16),
            v((128, RED), BF16),
            v((144, RED), BF16),
            v((128, RED), BF16),
            v((144, RED), BF16),
            v((272, RED), BF16),
            v((272, RED), BF16),
            v((4, 272, RED), BF16),
            v((RED, 256), BF16),
            v((RED, 16), BF16),
            v((272, RED), BF16),
            v((8, PART), F32),
            v((2, RED, PART), F32),
            v((2, 2, RED, NC), BF16),
            v((2, 2, RED, NC), BF16),
            v((2, 2, 4, 4, 32, NC), BF16),
            v((2, 2, 2, 2, 32, NC), BF16),
            v((2, 2, 2, 2, 32, NC), BF16),
            v((2, 2, 2, 4, 32, NC), BF16),
            v((2, 2, 4, 4, 8, NC), BF16),
            v((62, 8, NC), BF16),
            dma((8,)),
            dma((1,)),
            dma((18,)),
            dma((1,)),
            dma((1,)),
            dma((1,)),
            dma((6,)),
            dma((1,)),
            dma((6,)),
            dma((1,)),
            dma((2, 2)),
            dma((1,)),
            dma((2, 2, 3)),
            dma((1,)),
            dma((1,)),
        ],
        compiler_params=pltpu.CompilerParams(
            collective_id=0, has_side_effects=True, vmem_limit_bytes=LIMIT
        ),
        name="step",
    )(plan, samples, directions, targets, jacobian_targets, weights)
    return sum(result[k].astype(F32) for k in range(4))[None]


def solution(mesh):
    torus = Mesh(mesh.devices.reshape(4, 4, 2, 2, 2), AXES)
    return jax.shard_map(
        shards,
        mesh=torus,
        in_specs=(
            P(DP, None),
            P(DP, None),
            P(DP, None, None),
            P(DP, None),
            P(DP, None),
            P("zh", None, None),
        ),
        out_specs=P("zh", DP, None),
        check_vma=False,
    )
```

```python
import jax
import jax.numpy as jnp
from jax import lax
from jax.experimental import pallas as pl
from jax.experimental.pallas import tpu as pltpu
from jax.sharding import Mesh
from jax.sharding import PartitionSpec as P

AXES = ("x", "y", "zl", "c", "zh")
DP = ("x", "y", "zl", "c")
F32 = jnp.float32
BF16 = jnp.bfloat16
MESH = pl.DeviceIdType.MESH

RED = 512
WIDTH = 8192
TAN = 128
MICRO = 4
POOL = 8
PART = WIDTH // 4
HALF = PART // 2
ROWS = 8 * TAN
NC = 512
JAC = 32.0
LIMIT = 60 * 1024 * 1024


def nn(a, b):
    return lax.dot_general(a, b, (((1,), (0,)), ((), ())), preferred_element_type=F32)


def nt(a, b):
    return lax.dot_general(a, b, (((1,), (1,)), ((), ())), preferred_element_type=F32)


def kernel(
    plan_hbm,
    samples_hbm,
    dirs_hbm,
    targets_hbm,
    jt_hbm,
    w_hbm,
    out,
    plan,
    samples,
    dirs,
    targets,
    wst,
    wb,
    jt,
    s32,
    d32,
    t32,
    xd,
    e_buf,
    et_buf,
    xt_buf,
    p32,
    pk,
    tan,
    s1,
    s2,
    jac,
    ox,
    sa,
    fa,
    fb,
    ca,
    cb,
    r1,
    r2,
    mb,
    mt,
    mxt,
    lm,
    pr,
    g,
    ds,
    dr,
    gst,
    f1,
    cmb,
    p1r,
    hst,
    like,
    lsem,
    wss,
    wrs,
    xss,
    xrs,
    rss,
    rrs,
    ass_,
    ars,
    dss,
    drs,
    p1s,
    p1q,
    p3s,
    p3q,
):
    x = lax.axis_index("x")
    y = lax.axis_index("y")
    zl = lax.axis_index("zl")
    c = lax.axis_index("c")
    zh = lax.axis_index("zh")
    z = 2 * zh + zl

    def dev(px=x, py=y, pzl=zl, pc=c, pzh=zh):
        return (px, py, pzl, pc, pzh)

    def xpeer(o):
        return lax.rem(x + o, 4)

    def ypeer(o):
        return lax.rem(y + o, 4)

    n1 = dev(pzl=1 - zl)
    n2 = dev(pzl=1 - zl, pzh=1 - zh)
    mate = dev(pc=1 - c)
    here = dev()

    def send(src, dst, ssem, rsem, where):
        copy = pltpu.make_async_remote_copy(
            src_ref=src, dst_ref=dst, send_sem=ssem, recv_sem=rsem, device_id=where, device_id_type=MESH
        )
        copy.start()

    def arrived(dst, rsem):
        pltpu.make_async_remote_copy(
            src_ref=dst, dst_ref=dst, send_sem=rsem, recv_sem=rsem, device_id=here, device_id_type=MESH
        ).wait_recv()

    def sent(like, ssem):
        pltpu.make_async_remote_copy(
            src_ref=like, dst_ref=like, send_sem=ssem, recv_sem=ssem, device_id=here, device_id_type=MESH
        ).wait_send()

    barrier = pltpu.get_barrier_semaphore()
    peers = [n1, n2, dev(pzh=1 - zh)]
    peers += [dev(px=xpeer(o)) for o in (1, 2, 3)]
    peers += [dev(py=ypeer(o)) for o in (1, 2, 3)]
    peers += [dev(pzl=a, pc=1 - c, pzh=b) for a in (zl, 1 - zl) for b in (zh, 1 - zh)]
    for peer in peers:
        pl.semaphore_signal(barrier, inc=1, device_id=peer, device_id_type=MESH)

    small = []
    pieces = ((plan_hbm, plan), (samples_hbm, samples), (dirs_hbm, dirs), (targets_hbm, targets))
    for k, (src, dst) in enumerate(pieces):
        small.append(pltpu.make_async_copy(src, dst, lsem.at[2 + k]))
        small[-1].start()
    mine = (x, y)
    for k in range(4):
        for kind in range(2):
            first = pl.multiple_of(PART * (3 - z) + 1024 * (k // 2) + 512 * c + 256 * (k % 2) + 128 * kind, 128)
            src = w_hbm.at[0, pl.ds(pl.multiple_of(128 * mine[kind], 128), 128), pl.ds(first, 128)]
            pltpu.make_async_copy(src, wst.at[k, kind], lsem.at[6]).start()
    own_w = pltpu.make_async_copy(
        w_hbm.at[0, :, pl.ds(pl.multiple_of(PART * z, PART), PART)], wb.at[zh], lsem.at[0]
    )
    own_w.start()
    own_j = pltpu.make_async_copy(jt_hbm, jt, lsem.at[1])
    own_j.start()

    for copy in small:
        copy.wait()
    s32[...] = samples[...].astype(F32)
    d32[...] = dirs[...].astype(F32)
    t32[...] = targets[...].astype(F32)
    xd[zl, MICRO:8, :] = jnp.zeros((8 - MICRO, RED + TAN), F32)
    for i in range(MICRO):
        at = plan[0, i]
        xd[zl, i : i + 1, 0:RED] = s32[pl.ds(at, 1), :]
        xd[zl, i : i + 1, RED : RED + TAN] = d32[pl.ds(at, 1), :]

    pltpu.make_async_copy(wst, wst, lsem.at[6]).wait()
    pl.semaphore_wait(barrier, len(peers))

    def wslice(layer, core, k, kind, place):
        rows = pl.ds(pl.multiple_of(128 * place, 128), 128)
        at = 1024 * (k // 2) + 512 * core + 256 * (k % 2) + 128 * kind
        return wb.at[layer, rows, pl.ds(pl.multiple_of(at, 128), 128)]

    for k in range(4):
        for kind in range(2):
            send(
                wst.at[k, kind],
                wslice(zh, c, k, kind, mine[kind]),
                wss.at[0],
                wrs.at[2 * k + kind],
                n2,
            )
        if k == 0:
            send(xd.at[zl], xd.at[zl], xss.at[0], xrs.at[0], n1)

    def from_z(k):
        for kind in range(2):
            piece = wslice(1 - zh, c, k, kind, mine[kind])
            arrived(piece, wrs.at[2 * k + kind])
            for o in (1, 3, 2):
                to = dev(px=xpeer(o)) if kind == 0 else dev(py=ypeer(o))
                send(piece, piece, wss.at[0], wrs.at[8 + 2 * k + (o == 2)], to)
            send(piece, piece, wss.at[0], wrs.at[16 + k // 2], mate)

    def relay(k):
        for group in ((1, 3), (2,)):
            arrived(wb.at[1 - zh, pl.ds(0, 128), pl.ds(0, 256 * len(group))], wrs.at[8 + 2 * k + len(group) % 2])
            for o in group:
                for kind in range(2):
                    piece = wslice(1 - zh, c, k, kind, lax.rem(mine[kind] + 4 - o, 4))
                    send(piece, piece, wss.at[0], wrs.at[16 + k // 2], mate)

    def chunk_at(n, core):
        return pl.multiple_of(1024 * n + 512 * core, NC)

    def from_mate(n):
        arrived(wb.at[1 - zh, :, pl.ds(chunk_at(n, 1 - c), NC)], wrs.at[16 + n])

    from_z(0)
    from_z(1)
    arrived(xd.at[1 - zl], xrs.at[0])
    for j in range(8):
        row = xd[j // 4, j % 4 : j % 4 + 1, RED : RED + TAN]
        level = lax.broadcasted_iota(jnp.int32, (RED, TAN), 0).astype(F32)
        hot = jnp.where(level == row, 1.0, 0.0)
        et_buf[:, TAN * j : TAN * (j + 1)] = hot.astype(BF16)
        e_buf[TAN * j : TAN * (j + 1), :] = jnp.transpose(hot).astype(BF16)
    x16 = jnp.concatenate([xd[0, 0:4, 0:RED], xd[1, 0:4, 0:RED], jnp.zeros((8, RED), F32)], axis=0)
    e_buf[ROWS : ROWS + 16, :] = x16.astype(BF16)
    xt_buf[...] = jnp.transpose(x16).astype(BF16)
    jac[...] = jnp.zeros_like(jac)
    own_w.wait()

    def slopes(linear, cols):
        squash = 1.0 / (1.0 + jnp.exp(-linear))
        slope = squash * (1.0 + linear * (1.0 - squash))
        s1[:, cols] = slope
        s2[:, cols] = squash * (1.0 - squash) * (2.0 + linear * (1.0 - 2.0 * squash))
        hidden = jnp.concatenate([linear * squash, jnp.zeros((8, NC), F32)], axis=0)
        tan[ROWS : ROWS + 16, cols] = hidden.astype(BF16)
        return slope

    def forward(start):
        cols = pl.ds(pl.multiple_of(start, NC), NC)
        halves = ((512, ROWS + 16), (0, 512))
        for low, high in halves:
            p32[low:high, :] = nn(e_buf[low:high, :], wb[0, :, cols])
        slope = slopes(p32[ROWS : ROWS + 8, :], cols)
        for low, high in halves:
            for j in range(low // TAN, low // TAN + 4):
                rows = slice(TAN * j, TAN * (j + 1))
                picked = p32[rows, :]
                pk[rows, cols] = picked.astype(BF16)
                tan[rows, cols] = (slope[j : j + 1, :] * picked).astype(BF16)
            jac[low:high, :] += nt(tan[low:high, cols], wb[1, :, cols])

    from_z(2)
    relay(0)
    from_z(3)
    relay(1)
    forward(chunk_at(0, c))
    relay(2)
    from_mate(0)
    forward(chunk_at(0, 1 - c))
    relay(3)
    forward(chunk_at(1, c))
    from_mate(1)

    own = 2 * zl + zh
    b1 = 2 * (1 - zl) + zh
    b2 = 2 * (1 - zl) + (1 - zh)
    bo = 2 * zl + (1 - zh)
    lo, hi = pl.ds(0, 128), pl.ds(128, 144)
    cols = pl.ds(chunk_at(1, 1 - c), NC)
    tail16 = slice(ROWS, ROWS + 16)
    for b, kind in ((bo, 0), (b1, 1), (b2, 2), (own, 3)):
        rows = pl.ds(pl.multiple_of(256 * b, 256), 256)
        if kind == 0:
            p32[0:272, :] = nn(jnp.concatenate([e_buf[rows, :], e_buf[tail16, :]], axis=0), wb[0, :, cols])
            slopes(p32[256:264, :], cols)
        else:
            p32[0:256, :] = nn(e_buf[rows, :], wb[0, :, cols])
        for e in range(2):
            half = pl.ds(pl.multiple_of(256 * b + 128 * e, 128), 128)
            picked = p32[128 * e : 128 * e + 128, :]
            pk[half, cols] = picked.astype(BF16)
            tan[half, cols] = (s1[pl.ds(2 * b + e, 1), cols] * picked).astype(BF16)
        if kind == 0:
            both = nt(jnp.concatenate([tan[rows, cols], tan[tail16, cols]], axis=0), wb[1, :, cols])
            done = jac[rows, :] + both[0:256, :]
            o16 = jac[tail16, :] + both[256:272, :]
            for k in range(4):
                o2 = jnp.concatenate([o16[2 * k : 2 * k + 2, :], jnp.zeros((14, RED), F32)], axis=0)
                ox[k] = o2
                sa[k, 256:272, :] = o2.astype(BF16)
        else:
            done = jac[rows, :] + nt(tan[rows, cols], wb[1, :, cols])
        if kind == 3:
            jac[rows, :] = done
        else:
            sa[b, 0:256, :] = done.astype(BF16)
        if kind == 0:
            send(sa.at[bo, lo], fa, rss.at[0], rrs.at[0], n1)
            send(sa.at[bo, hi], fb, rss.at[0], rrs.at[1], n2)
        elif kind == 1:
            send(sa.at[b1, lo], r1.at[lo], rss.at[0], rrs.at[2], n1)
        elif kind == 2:
            send(sa.at[b2, hi], r2.at[hi], rss.at[0], rrs.at[3], n2)
    arrived(fa, rrs.at[0])
    ca[...] = (sa[b2, 0:128, :].astype(F32) + fa[...].astype(F32)).astype(BF16)
    send(ca, r2.at[lo], rss.at[0], rrs.at[4], n2)
    arrived(fb, rrs.at[1])
    cb[...] = (sa[b1, 128:272, :].astype(F32) + fb[...].astype(F32)).astype(BF16)
    send(cb, r1.at[hi], rss.at[0], rrs.at[5], n1)

    own_j.wait()
    arrived(r1.at[lo], rrs.at[2])
    arrived(r2.at[lo], rrs.at[4])
    p0 = plan[0, 2 * zh]
    p1 = plan[0, 2 * zh + 1]
    full = jac[pl.ds(pl.multiple_of(256 * own, 256), 128), :]
    full = full + r1[0:128, :].astype(F32) + r2[0:128, :].astype(F32)
    mb[own, 0:128, :] = (JAC * (full - jt[p0].astype(F32))).astype(BF16)
    send(mb.at[own, lo], mb.at[own, lo], ass_.at[0], ars.at[0], n1)
    arrived(r2.at[hi], rrs.at[3])
    arrived(r1.at[hi], rrs.at[5])
    full = jac[pl.ds(pl.multiple_of(256 * own + 128, 128), 128), :]
    full = full + r1[128:256, :].astype(F32) + r2[128:256, :].astype(F32)
    mb[own, 128:256, :] = (JAC * (full - jt[p1].astype(F32))).astype(BF16)
    full = ox[own] + r1[256:272, :].astype(F32) + r2[256:272, :].astype(F32)
    goal = jnp.concatenate([t32[pl.ds(p0, 1), :], t32[pl.ds(p1, 1), :], jnp.zeros((14, RED), F32)], axis=0)
    mb[own, 256:272, :] = (full - goal).astype(BF16)
    send(mb.at[own, hi], mb.at[own, hi], ass_.at[0], ars.at[3], n2)
    send(mb.at[own, lo], mb.at[own, lo], ass_.at[0], ars.at[1], n2)
    send(mb.at[own, hi], mb.at[own, hi], ass_.at[0], ars.at[2], n1)

    def ends(pair):
        return [(b, 128 * e, pl.ds(pl.multiple_of(256 * b + 128 * e, 128), 128), 2 * b + e) for b, e in pair]

    def turn(pair, some=(0, 1)):
        for k, (b, at, _, _) in enumerate(ends(pair)):
            if k not in some:
                continue
            mt[:, 128 * k : 128 * k + 128] = jnp.transpose(mb[b, at : at + 128, :])
            lm[128 * k : 128 * k + 128, :] = mb[b, at : at + 128, :]

    def picked_grads(pair, cot, cols):
        parts = []
        for k, (_, _, rows, j) in enumerate(ends(pair)):
            ct = cot[128 * k : 128 * k + 128, :].astype(BF16).astype(F32)
            pr[pl.ds(j, 1), cols] = jnp.sum(ct * pk[rows, cols].astype(F32), axis=0, keepdims=True)
            parts.append((ct * s1[pl.ds(j, 1), cols]).astype(BF16))
        return jnp.concatenate(parts, axis=0)

    def tangents(pair, cols):
        return jnp.concatenate([tan[rows, cols] for _, _, rows, _ in ends(pair)], axis=0)

    def hot_columns(pair):
        return jnp.concatenate([et_buf[:, rows] for _, _, rows, _ in ends(pair)], axis=1)

    def add_to(layer, cols, new, first=False):
        g[layer, :, cols] = new if first else g[layer, :, cols] + new

    def backward(pair, first):
        turn(pair)
        chunks = [pl.ds(NC * n, NC) for n in range(PART // NC)]

        def cotangents(n):
            p32[512 * (n % 2) : 512 * (n % 2) + 256, :] = nn(lm[0:256, :], wb[1, :, chunks[n]])

        cotangents(0)
        for n, cols in enumerate(chunks):
            if n + 1 < len(chunks):
                cotangents(n + 1)
            add_to(1, cols, nn(mt[...], tangents(pair, cols)), first)
            r = picked_grads(pair, p32[512 * (n % 2) : 512 * (n % 2) + 256, :], cols)
            add_to(0, cols, nn(hot_columns(pair), r), first)

    backward(((own, 0), (own, 1)), True)
    arrived(mb.at[b1, lo], ars.at[0])
    send(mb.at[b1, lo], mb.at[b1, lo], ass_.at[0], ars.at[4], n2)
    arrived(mb.at[b2, hi], ars.at[3])
    send(mb.at[b2, hi], mb.at[b2, hi], ass_.at[0], ars.at[5], n1)
    backward(((b1, 0), (b2, 1)), False)
    arrived(mb.at[b2, lo], ars.at[1])
    arrived(mb.at[b1, hi], ars.at[2])
    backward(((b1, 1), (b2, 0)), False)
    tail = ((bo, 0), (bo, 1))
    arrived(mb.at[bo, lo], ars.at[4])
    turn(tail, (0,))
    arrived(mb.at[bo, hi], ars.at[5])
    turn(tail, (1,))

    heads = [mb[b, 256:272, :].astype(F32)[0:2, :] for b in range(4)]
    m16 = jnp.concatenate(heads + [jnp.zeros((8, RED), F32)], axis=0)
    lm[256:272, :] = m16.astype(BF16)
    mxt[...] = jnp.transpose(m16).astype(BF16)

    def ahead(layer):
        return xpeer(1) if layer == 1 else ypeer(1)

    def behind(layer):
        return xpeer(3) if layer == 1 else ypeer(3)

    def at_place(layer, place):
        return dev(px=place) if layer == 1 else dev(py=place)

    def half_for(q, layer, place, part):
        if layer == 1:
            return gst.at[q, layer, place, pl.ds(2 * part, 2)]
        return gst.at[q, layer, pl.ds(2 * part, 2), place]

    def rows_for(layer, place, k):
        at = 128 * place + 32 * k if layer == 1 else 128 * k + 32 * place
        return pl.ds(pl.multiple_of(at, 32), 32)

    def start_unit(q, layer, steps):
        across = xpeer(2) if layer == 1 else ypeer(2)
        up, down = ahead(layer), behind(layer)
        moves = (
            (half_for(q, layer, across, 0), f1.at[q, layer, 0], up),
            (half_for(q, layer, across, 1), f1.at[q, layer, 1], down),
            (half_for(q, layer, up, 1), p1r.at[q, layer, 0, pl.ds(2, 2)], up),
            (half_for(q, layer, down, 0), p1r.at[q, layer, 1, pl.ds(0, 2)], down),
        )
        for k in steps:
            src, dst, place = moves[k]
            send(src, dst, p1s.at[0], p1q.at[q, layer, min(k, 2)], at_place(layer, place))

    def forward_unit(q, layer):
        cols = pl.ds(pl.multiple_of(HALF * c + NC * q, NC), NC)
        for part, place in ((0, ahead(layer)), (1, behind(layer))):
            arrived(f1.at[q, layer, part], p1q.at[q, layer, part])
            for k in range(2):
                total = g[layer, rows_for(layer, place, 2 * part + k), cols]
                cmb[q, layer, part, k] = (total + f1[q, layer, part, k].astype(F32)).astype(BF16)
            send(
                cmb.at[q, layer, part],
                p1r.at[q, layer, part, pl.ds(2 * part, 2)],
                p1s.at[0],
                p1q.at[q, layer, 2],
                at_place(layer, place),
            )

    units = []
    for half in range(2):
        for q in range(2):
            base = HALF * (1 - c) if half == 0 else HALF * c
            units.append((half, q, pl.ds(pl.multiple_of(base + NC * q, NC), NC)))

    def leave(half, q, layer, cols, total):
        if half == 0:
            ds[q, layer] = (g[layer, :, cols] + total).astype(BF16)
            send(ds.at[q, layer], dr.at[q, layer], dss.at[0], drs.at[q, layer], mate)
        else:
            g[layer, :, cols] += total

    def tail_cotangents(n):
        p32[512 * (n % 2) : 512 * (n % 2) + 272, :] = nn(lm[...], wb[1, :, units[n][2]])

    tail_cotangents(0)
    for n, (half, q, cols) in enumerate(units):
        if n + 1 < len(units):
            tail_cotangents(n + 1)
        total = nn(mt[...], tangents(tail, cols)) + nn(mxt[...], tan[tail16, cols])
        leave(half, q, 1, cols, total)
        at = 512 * (n % 2)
        r = picked_grads(tail, p32[at : at + 256, :], cols)
        cx = p32[at + 256 : at + 264, :].astype(BF16).astype(F32)
        pre = cx * s1[:, cols] + s2[:, cols] * pr[:, cols]
        pre = jnp.concatenate([pre, jnp.zeros((8, NC), F32)], axis=0).astype(BF16)
        leave(half, q, 0, cols, nn(hot_columns(tail), r) + nn(xt_buf[...], pre))
        if half == 0:
            continue
        for layer in (1, 0):
            arrived(dr.at[q, layer], drs.at[q, layer])
            total = g[layer, :, cols] + dr[q, layer].astype(F32)
            g[layer, :, cols] = total
            gst[q, layer] = total.astype(BF16).reshape(4, 4, 32, NC)
            start_unit(q, layer, range(4) if q == 0 else range(2))

    def cols_at(place, q):
        return pl.ds(pl.multiple_of(HALF * place + NC * q, NC), NC)

    for layer in (1, 0):
        forward_unit(0, layer)
        start_unit(1, layer, range(2, 4))
    for layer in (1, 0):
        forward_unit(1, layer)
    for q in range(2):
        cols = pl.ds(pl.multiple_of(HALF * c + NC * q, NC), NC)
        for layer in (1, 0):
            arrived(p1r.at[q, layer], p1q.at[q, layer, 2])
            for k in range(4):
                total = g[layer, rows_for(layer, x if layer == 1 else y, k), cols]
                for side in range(2):
                    total = total + p1r[q, layer, side, k].astype(F32)
                for part in range(4):
                    hst[q, layer, k, part] = total[8 * part : 8 * part + 8, :].astype(BF16)
            ring = y if layer == 1 else x
            slot = out.at[ring, :, cols_at(2 * z + c, q)]
            for o in (2, 1, 3, 0):
                place = lax.rem(ring + o, 4)
                for a, b in ((1, 1), (1, 0), (0, 1), (0, 0)):
                    pzl, pc = lax.rem(zl + a, 2), lax.rem(c + b, 2)
                    src = hst.at[q, layer, place, 2 * pzl + pc]
                    to = dev(pzl=pzl, pc=pc, pzh=layer)
                    to = (to[0], place, *to[2:]) if layer == 1 else (place, *to[1:])
                    if o + a + b:
                        send(src, slot, p3s.at[0], p3q.at[0], to)
                        continue

                    @pl.when(zh != layer)
                    def _():
                        send(src, slot, p3s.at[0], p3q.at[0], to)

                    @pl.when(zh == layer)
                    def _():
                        pltpu.make_async_copy(src, slot, lsem.at[7]).start()

    arrived(like, p3q.at[0])
    sent(wb.at[0], wss.at[0])
    sent(xd.at[0], xss.at[0])
    sent(sa.at[pl.ds(0, 3)], rss.at[0])
    sent(mb.at[pl.ds(0, 3)], ass_.at[0])
    sent(ds, dss.at[0])
    sent(gst.at[:, :, pl.ds(0, 3)], p1s.at[0])
    sent(like, p3s.at[0])
    pltpu.make_async_copy(like.at[0:2], like.at[0:2], lsem.at[7]).wait()


def shards(samples, targets, jacobian_targets, directions, plan, weights):
    anywhere = pl.BlockSpec(memory_space=pl.ANY)
    dma = pltpu.SemaphoreType.DMA
    v = pltpu.VMEM
    result = pl.pallas_call(
        kernel,
        out_shape=jax.ShapeDtypeStruct((4, 8, WIDTH), BF16),
        in_specs=[anywhere] * 6,
        out_specs=anywhere,
        scratch_shapes=[
            pltpu.SMEM((1, POOL), jnp.int32),
            v((POOL, RED), BF16),
            v((POOL, TAN), jnp.int32),
            v((POOL, RED), BF16),
            v((4, 2, 128, 128), BF16),
            v((2, RED, PART), BF16),
            v((POOL, TAN, RED), BF16),
            v((POOL, RED), F32),
            v((POOL, TAN), F32),
            v((POOL, RED), F32),
            v((2, 8, RED + TAN), F32),
            v((ROWS + 16, RED), BF16),
            v((RED, ROWS), BF16),
            v((RED, 16), BF16),
            v((ROWS + 16, NC), F32),
            v((ROWS, PART), BF16),
            v((ROWS + 16, PART), BF16),
            v((8, PART), F32),
            v((8, PART), F32),
            v((ROWS + 16, RED), F32),
            v((4, 16, RED), F32),
            v((4, 272, RED), BF16),
            v((128, RED), BF16),
            v((144, RED), BF16),
            v((128, RED), BF16),
            v((144, RED), BF16),
            v((272, RED), BF16),
            v((272, RED), BF16),
            v((4, 272, RED), BF16),
            v((RED, 256), BF16),
            v((RED, 16), BF16),
            v((272, RED), BF16),
            v((8, PART), F32),
            v((2, RED, PART), F32),
            v((2, 2, RED, NC), BF16),
            v((2, 2, RED, NC), BF16),
            v((2, 2, 4, 4, 32, NC), BF16),
            v((2, 2, 2, 2, 32, NC), BF16),
            v((2, 2, 2, 2, 32, NC), BF16),
            v((2, 2, 2, 4, 32, NC), BF16),
            v((2, 2, 4, 4, 8, NC), BF16),
            v((62, 8, NC), BF16),
            dma((8,)),
            dma((1,)),
            dma((18,)),
            dma((1,)),
            dma((1,)),
            dma((1,)),
            dma((6,)),
            dma((1,)),
            dma((6,)),
            dma((1,)),
            dma((2, 2)),
            dma((1,)),
            dma((2, 2, 3)),
            dma((1,)),
            dma((1,)),
        ],
        compiler_params=pltpu.CompilerParams(
            collective_id=0, has_side_effects=True, vmem_limit_bytes=LIMIT
        ),
        name="step",
    )(plan, samples, directions, targets, jacobian_targets, weights)
    return sum(result[k].astype(F32) for k in range(4))[None]


def solution(mesh):
    torus = Mesh(mesh.devices.reshape(4, 4, 2, 2, 2), AXES)
    return jax.shard_map(
        shards,
        mesh=torus,
        in_specs=(
            P(DP, None),
            P(DP, None),
            P(DP, None, None),
            P(DP, None),
            P(DP, None),
            P("zh", None, None),
        ),
        out_specs=P("zh", DP, None),
        check_vma=False,
    )
```
